128 devices in a mesh: space: 16 (over z_lo, y, core), group: 8 (over z_hi, x).
Axes of the slice: x: 4, y: 4, z: 4 (z_hi: 2, z_lo: 2; z = z_hi * 2 + z_lo), core: 2. Of those that a mesh axis runs over, the one named last changes fastest.
Arguments:
- snapshot_basis: bfloat16 [131072, 2048], P('space', 'group'), may hold values from -40 to 40
- sketch: float32 [3, 512, 256], replicated, may hold values from -0.25 to 0.25
Outputs:
- merged_basis: bfloat16 [131072, 256], P(('space', 'group'))
The draws below stay inside these ranges and needn't reach their ends.
All inputs are finite; a program needn't handle non-finite values.
Results may differ from the reference program's by a relative error of at most 0.0067.
Values may be sent and summed in bfloat16 or wider, within the bound.
A program may use at most 128 MiB of HBM per device.

```python
import jax
import jax.numpy as jnp
from jax import lax

K = 256
STEPS = 5
ROWS_DEV = 8192
ROWS = 131072
COLS = 2048
LEVELS = 3
N_GROUP = 8


def draw_snapshot_basis(key, part):
    key_scale = jax.random.fold_in(key, 11)
    key_entry = jax.random.fold_in(key, 12)
    slabs = ROWS // ROWS_DEV
    logs = jax.random.uniform(key_scale, (slabs, 1, COLS), jnp.float32, jnp.log(0.1), jnp.log(1.5))
    scales = jnp.exp(logs)
    ramp = jnp.exp(jnp.log(3.0) * jnp.arange(ROWS, dtype=jnp.float32) / ROWS)
    ramp = ramp.reshape(slabs, ROWS_DEV, 1)
    entries = jax.random.normal(key_entry, (ROWS, COLS), jnp.float32)
    base = jnp.clip(entries, -6.0, 6.0).reshape(slabs, ROWS_DEV, COLS)
    values = base * scales * ramp
    return values.reshape(ROWS, COLS).astype(jnp.bfloat16)


def normal_values(own_key, extent, deviation, bound, kind=jnp.bfloat16):
    result = deviation * jax.random.normal(own_key, extent, jnp.float32)
    return jnp.clip(result, min=-bound, max=bound).astype(kind)


def setup_inputs(seed: int = 0) -> dict:
    key_list = jax.random.split(jax.random.key(seed), 3)
    snapshot_basis = draw_snapshot_basis(jax.random.fold_in(key_list[2], 71), 0)
    sketch = normal_values(key_list[1], (LEVELS, 2 * K, K), (2 * K) ** -0.5, 0.25, jnp.float32)
    return dict(snapshot_basis=snapshot_basis, sketch=sketch)


def filter_mix(gram, sketch_level):
    width = gram.shape[0]
    eye = jnp.eye(width, dtype=jnp.float32)
    scaled = gram / (jnp.trace(gram) / width)
    shifted = scaled - eye
    iterate = shifted / (1.0 + jnp.sqrt(jnp.sum(shifted * shifted)))
    for step in range(STEPS):
        square = jnp.dot(iterate, iterate, precision=lax.Precision.HIGHEST)
        cube = jnp.dot(square, iterate, precision=lax.Precision.HIGHEST)
        iterate = 1.5 * iterate - 0.5 * cube
    applied = jnp.dot(iterate, sketch_level, precision=lax.Precision.HIGHEST)
    return (0.5 * (sketch_level + applied)).astype(jnp.bfloat16)

def merge_pair(lower, upper, sketch_level):
    stacked = jnp.concatenate([lower, upper], axis=1)
    gram = lax.dot_general(stacked, stacked, (((0,), (0,)), ((), ())), preferred_element_type=jnp.float32)
    mix = filter_mix(gram, sketch_level)
    return jnp.dot(stacked, mix, preferred_element_type=jnp.float32).astype(jnp.bfloat16)

def reference(snapshot_basis, sketch):
    panels = [snapshot_basis[:, g * K:(g + 1) * K] for g in range(N_GROUP)]
    for level in range(LEVELS):
        reach = 2 ** level
        fresh = list(panels)
        for lower in range(N_GROUP):
            if lower >> level & 1 == 0:
                merged = merge_pair(panels[lower], panels[lower + reach], sketch[level])
                fresh[lower] = merged
                fresh[lower + reach] = merged
        panels = fresh
    return panels[0]
```

```python
import functools

import jax
import jax.numpy as jnp
from jax import lax
from jax.experimental import pallas as pl
from jax.experimental.pallas import tpu as pltpu
from jax.sharding import PartitionSpec as P

STEPS = 5
MESH = pl.DeviceIdType.MESH
F32 = jnp.float32
BF16 = jnp.bfloat16
CHUNKS = 8
ORDER = ((2, 1), (1, 1), (3, 1), (0, 1), (2, 0), (1, 0), (3, 0))


def dot(a, b):
    return jnp.dot(a, b, preferred_element_type=F32)


def dot_t(a, b):
    return lax.dot_general(a, b, (((0,), (0,)), ((), ())), preferred_element_type=F32)


def split(a):
    high = a.astype(BF16)
    return high, (a - high.astype(F32)).astype(BF16)


def loop(low, high, body):
    def step(i, carry):
        body(i)
        return carry

    lax.fori_loop(low, high, step, 0)


def start_of_filter(gram):
    width = gram.shape[0]
    row = lax.broadcasted_iota(jnp.int32, gram.shape, 0)
    col = lax.broadcasted_iota(jnp.int32, gram.shape, 1)
    eye = row == col
    trace = jnp.sum(jnp.where(eye, gram, 0.0), axis=(0, 1), keepdims=True)
    shifted = gram * (1.0 / (trace / width)) - jnp.where(eye, 1.0, 0.0)
    norm = jnp.sqrt(jnp.sum(shifted * shifted, axis=(0, 1), keepdims=True))
    return shifted * (1.0 / (1.0 + norm))


def filter_step(iterate):
    low = iterate.astype(BF16)
    square = dot(low, low).astype(BF16)
    return 1.5 * iterate - 0.5 * dot(square, low)


def mix_of(iterate, sketch):
    return (0.5 * (sketch + dot(iterate.astype(BF16), sketch.astype(BF16)))).astype(BF16)


def projected(gram, mix):
    high, low = split(gram)
    half = dot(high, mix) + dot(low, mix)
    high, low = split(half)
    return dot_t(mix, high) + dot_t(mix, low)


def kernel(
    n_space, n_group,
    x_hbm, sk_hbm, out_ref,
    panels, own, sketch, diag, diag_in, diag_all,
    cs0, cr0, cg0, ca0, cs1, cr1, cg1, ca1, cs2, cr2, cg2, ca2,
    gram0, gram1, gram2, it0, it1, mix0, mix1, p1, p2, block2,
    a_send, a_recv, l_sem, dr_send, dr_recv, dg_send, dg_recv, da_send, da_recv,
    r_send, r_recv, g_send, g_recv, k_send, k_recv, c_send, c_recv,
):
    s = lax.axis_index("space")
    g = lax.axis_index("group")
    width = x_hbm.shape[1]
    block = x_hbm.shape[0] // n_group
    n_k = n_space // 2
    k = lax.div(s, 2)
    c = lax.rem(s, 2)
    gx = lax.rem(g, 4)
    gz = lax.div(g, 4)
    part = width // n_k
    partner = 2 * k + 1 - c

    def remote(src, dst, send, recv, to):
        return pltpu.make_async_remote_copy(
            src_ref=src, dst_ref=dst, send_sem=send, recv_sem=recv,
            device_id=to, device_id_type=MESH,
        )

    def group_peer(d):
        return s, lax.rem(g + d, n_group)

    def space_peer(d):
        return lax.rem(s + d, n_space), g

    def core_peer(d):
        return 2 * lax.rem(k + d, n_k) + c, g

    barrier = pltpu.get_barrier_semaphore()
    loop(1, n_group, lambda d: pl.semaphore_signal(
        barrier, inc=1, device_id=group_peer(d), device_id_type=MESH))
    loop(1, n_space, lambda d: pl.semaphore_signal(
        barrier, inc=1, device_id=space_peer(d), device_id_type=MESH))

    whole = pltpu.make_async_copy(x_hbm, own, l_sem.at[0])
    whole.start()
    mine = pltpu.make_async_copy(
        x_hbm.at[pl.ds(pl.multiple_of(g * block, block), block)], panels.at[g], l_sem.at[1])
    mine.start()
    tests = pltpu.make_async_copy(sk_hbm, sketch, l_sem.at[2])
    tests.start()
    pl.semaphore_wait(barrier, n_group - 1 + n_space - 1)

    piece = block // CHUNKS

    def panel_copy(i, at, size):
        dx, dz = ORDER[i]
        to = lax.rem(gz + dz, 2) * 4 + lax.rem(gx + dx, 4)
        return remote(
            x_hbm.at[pl.ds(pl.multiple_of(to * block + at, size), size)],
            panels.at[g, pl.ds(pl.multiple_of(at, size), size)],
            a_send.at[i], a_recv.at[i], (s, to))

    def send_pieces(ch):
        for i in range(len(ORDER)):
            panel_copy(i, ch * piece, piece).start()

    loop(0, CHUNKS // 2, send_pieces)

    whole.wait()
    diag[...] = jnp.zeros_like(diag)

    def add_diag(j):
        rows = own[pl.ds(pl.multiple_of(j * block, block), block), :]
        diag[...] += dot_t(rows, rows)

    loop(0, n_group, add_diag)

    def diag_copy(d):
        to = lax.rem(k + d, n_k)
        return remote(
            diag.at[pl.ds(pl.multiple_of(to * part, part), part)], diag_in.at[s],
            dr_send.at[d], dr_recv.at[s], (2 * to + gz, g))

    keeps = c == gz
    loop(1, n_k, lambda d: diag_copy(d).start())

    @pl.when(jnp.logical_not(keeps))
    def _():
        diag_copy(0).start()

    @pl.when(keeps)
    def _():
        diag_in[s] = diag[pl.ds(pl.multiple_of(k * part, part), part), :]

        def arrived(d):
            at = lax.rem(s + d, n_space)
            remote(diag.at[pl.ds(0, part)], diag_in.at[at], dr_send.at[0], dr_recv.at[at],
                   (at, g)).wait_recv()

        loop(1, n_space, arrived)
        diag_all[k, gx] = jnp.sum(diag_in[...], axis=0)

        def pass_on(d):
            remote(diag_all.at[k, gx], diag_all.at[k, gx], dg_send.at[d], dg_recv.at[gx],
                   group_peer(d)).start()

        loop(1, n_group, pass_on)

    loop(CHUNKS // 2, CHUNKS, send_pieces)

    def diag_arrived(j):
        @pl.when(4 * c + j != g)
        def _():
            remote(diag_all.at[k, j], diag_all.at[k, j], dg_send.at[0], dg_recv.at[j],
                   (s, 4 * c + j)).wait_recv()

    loop(0, 4, diag_arrived)

    def diag_gather(d):
        return remote(diag_all.at[k], diag_all.at[k], da_send.at[d], da_recv.at[d], core_peer(d))

    loop(1, n_k, lambda d: diag_gather(d).start())

    def reduce_cross(level, cs, cr, cg, ca, everyone, beside):
        def scatter(d):
            to = lax.rem(s + d, n_space)
            return remote(cs.at[to], cr.at[s], r_send.at[level, d], r_recv.at[level, d], (to, g))

        def share(d):
            return remote(cg.at[g], cg.at[g], g_send.at[level, d], g_recv.at[level, d],
                          group_peer(d))

        at = s if everyone else k
        peers = n_space if everyone else n_k

        def gather(d):
            return remote(ca.at[at], ca.at[at], k_send.at[level, d], k_recv.at[level, d],
                          space_peer(d) if everyone else core_peer(d))

        loop(1, n_space, lambda d: scatter(d).start())
        cr[s] = cs[s]
        beside()
        loop(1, n_space, lambda d: scatter(d).wait_recv())
        cg[g] = jnp.sum(cr[...].astype(F32), axis=0).astype(BF16)
        loop(1, n_group, lambda d: share(d).start())
        loop(1, n_group, lambda d: share(d).wait_recv())
        ca[at] = jnp.sum(cg[...].astype(F32), axis=0).astype(BF16)
        loop(1, peers, lambda d: gather(d).start())
        loop(1, peers, lambda d: gather(d).wait_recv())

        def sent():
            loop(1, n_space, lambda d: scatter(d).wait_send())
            loop(1, n_group, lambda d: share(d).wait_send())
            loop(1, peers, lambda d: gather(d).wait_send())

        return sent

    def apply_mix(src, a, b, mix, dst, at):
        upper, lower = mix[:width, :], mix[width:, :]
        tile = 256

        def rows(j):
            here = pl.ds(pl.multiple_of(j * tile, tile), tile)
            dst[at, here, :] = (dot(src[a, here, :], upper) + dot(src[b, here, :], lower)).astype(BF16)

        loop(0, block // tile, rows)

    def fill(gram, at, cross):
        gram[at, :width, width:] = cross
        gram[at, width:, :width] = cross.T

    mine.wait()
    for i in range(len(ORDER)):
        panel_copy(i, 0, block).wait_recv()
    for p in range(4):
        cross = dot_t(panels[2 * p], panels[2 * p + 1]).astype(BF16).reshape(n_k, part, width)
        for kk in range(n_k):
            cs0[2 * kk + p // 2, p % 2] = cross[kk]

    def beside0():
        loop(1, n_k, lambda d: diag_gather(d).wait_recv())
        for i in range(2):
            gram0[i, :width, :width] = diag_all[:, 2 * i].reshape(width, width)
            gram0[i, width:, width:] = diag_all[:, 2 * i + 1].reshape(width, width)

    sent0 = reduce_cross(0, cs0, cr0, cg0, ca0, False, beside0)
    for i in range(2):
        fill(gram0, i, ca0[:, i].astype(F32).reshape(width, width))
        it0[i] = start_of_filter(gram0[i])

    def steps0(_):
        for i in range(2):
            it0[i] = filter_step(it0[i])

    loop(0, STEPS, steps0)
    tests.wait()
    for i in range(2):
        mix0[2 * c + i] = mix_of(it0[i], sketch[0])
    swap0 = remote(mix0.at[pl.ds(2 * c, 2)], mix0.at[pl.ds(2 * c, 2)], c_send.at[0], c_recv.at[0],
                   (partner, g))
    swap0.start()

    for i in range(2):
        pair = 2 * c + i
        apply_mix(panels, 2 * pair, 2 * pair + 1, mix0[pair], p1, pair)
    swap0.wait_recv()
    for i in range(2):
        pair = 2 * (1 - c) + i
        apply_mix(panels, 2 * pair, 2 * pair + 1, mix0[pair], p1, pair)
    for q in range(2):
        cross = dot_t(p1[2 * q], p1[2 * q + 1]).astype(BF16).reshape(n_k, part, width)
        for kk in range(n_k):
            cs1[2 * kk + q] = cross[kk]

    def beside1():
        gram1[0, :width, :width] = projected(gram0[0], mix0[2 * c])
        gram1[0, width:, width:] = projected(gram0[1], mix0[2 * c + 1])

    sent1 = reduce_cross(1, cs1, cr1, cg1, ca1, False, beside1)
    fill(gram1, 0, ca1[...].astype(F32).reshape(width, width))
    it1[...] = start_of_filter(gram1[0])

    def steps1(_):
        it1[...] = filter_step(it1[...])

    loop(0, STEPS, steps1)
    mix1[c] = mix_of(it1[...], sketch[1])
    swap1 = remote(mix1.at[c], mix1.at[c], c_send.at[1], c_recv.at[1], (partner, g))
    swap1.start()

    apply_mix(p1, 2 * c, 2 * c + 1, mix1[c], p2, c)
    swap1.wait_recv()
    apply_mix(p1, 2 * (1 - c), 2 * (1 - c) + 1, mix1[1 - c], p2, 1 - c)
    cross = dot_t(p2[0], p2[1]).astype(BF16).reshape(n_space, width // n_space, width)
    cs2[...] = cross
    swap2 = remote(block2.at[c], block2.at[c], c_send.at[2], c_recv.at[2], (partner, g))

    def beside2():
        block2[c] = projected(gram1[0], mix1[c])
        swap2.start()

    sent2 = reduce_cross(2, cs2, cr2, cg2, ca2, True, beside2)
    swap2.wait_recv()
    gram2[0, :width, :width] = block2[0]
    gram2[0, width:, width:] = block2[1]
    fill(gram2, 0, ca2[...].astype(F32).reshape(width, width))
    it1[...] = start_of_filter(gram2[0])
    loop(0, STEPS, steps1)
    last = mix_of(it1[...], sketch[2])
    upper, lower = last[:width, :], last[width:, :]
    tile = 256

    def rows(j):
        here = pl.ds(pl.multiple_of(j * tile, tile), tile)
        out_ref[here, :] = (dot(p2[0, here, :], upper) + dot(p2[1, here, :], lower)).astype(BF16)

    loop(0, block // tile, rows)

    for i in range(len(ORDER)):
        panel_copy(i, 0, block).wait_send()
    loop(1, n_k, lambda d: diag_copy(d).wait_send())

    @pl.when(jnp.logical_not(keeps))
    def _():
        diag_copy(0).wait_send()

    @pl.when(keeps)
    def _():
        loop(1, n_group, lambda d: remote(
            diag_all.at[k, gx], diag_all.at[k, gx], dg_send.at[d], dg_recv.at[gx],
            group_peer(d)).wait_send())

    loop(1, n_k, lambda d: diag_gather(d).wait_send())
    sent0()
    sent1()
    sent2()
    for swap in (swap0, swap1, swap2):
        swap.wait_send()


def body(n_space, n_group, snapshot_basis, sketch):
    rows, width = snapshot_basis.shape
    block = rows // n_group
    n_k = n_space // 2
    part = width // n_k
    dma = pltpu.SemaphoreType.DMA
    vmem = pltpu.VMEM
    scratch = [
        vmem((n_group, block, width), BF16), vmem((rows, width), BF16), vmem(sketch.shape, F32),
        vmem((width, width), F32), vmem((n_space, part, width), F32), vmem((n_k, 4, part, width), F32),
        vmem((n_space, 2, part, width), BF16), vmem((n_space, 2, part, width), BF16),
        vmem((n_group, 2, part, width), BF16), vmem((n_k, 2, part, width), BF16),
        vmem((n_space, part, width), BF16), vmem((n_space, part, width), BF16),
        vmem((n_group, part, width), BF16), vmem((n_k, part, width), BF16),
        vmem((n_space, part // 2, width), BF16), vmem((n_space, part // 2, width), BF16),
        vmem((n_group, part // 2, width), BF16), vmem((n_space, part // 2, width), BF16),
        vmem((2, 2 * width, 2 * width), F32), vmem((1, 2 * width, 2 * width), F32),
        vmem((1, 2 * width, 2 * width), F32),
        vmem((2, 2 * width, 2 * width), F32), vmem((2 * width, 2 * width), F32),
        vmem((4, 2 * width, width), BF16), vmem((2, 2 * width, width), BF16),
        vmem((4, block, width), BF16), vmem((2, block, width), BF16), vmem((2, width, width), F32),
        dma((len(ORDER),)), dma((len(ORDER),)), dma((3,)),
        dma((n_k,)), dma((n_space,)), dma((n_group,)), dma((4,)), dma((n_k,)), dma((n_k,)),
        dma((3, n_space)), dma((3, n_space)), dma((3, n_group)), dma((3, n_group)),
        dma((3, n_space)), dma((3, n_space)), dma((3,)), dma((3,)),
    ]
    return pl.pallas_call(
        functools.partial(kernel, n_space, n_group),
        out_shape=jax.ShapeDtypeStruct((block, width), BF16),
        in_specs=[pl.BlockSpec(memory_space=pl.ANY)] * 2,
        out_specs=pl.BlockSpec(memory_space=pltpu.VMEM),
        scratch_shapes=scratch,
        compiler_params=pltpu.CompilerParams(
            collective_id=0, has_side_effects=True, vmem_limit_bytes=56 * 1024 * 1024),
        name="merge",
    )(snapshot_basis, sketch)


def solution(mesh):
    in_specs = (P("space", "group"), P())
    out_specs = P(("space", "group"), None)
    step = functools.partial(body, mesh.shape["space"], mesh.shape["group"])
    return jax.shard_map(step, mesh=mesh, in_specs=in_specs, out_specs=out_specs, check_vma=False)
```

```python
import functools

import jax
import jax.numpy as jnp
from jax import lax
from jax.experimental import pallas as pl
from jax.experimental.pallas import tpu as pltpu
from jax.sharding import PartitionSpec as P

STEPS = 5
MESH = pl.DeviceIdType.MESH
F32 = jnp.float32
BF16 = jnp.bfloat16
SPAN = 4
PIECES = 4
SPLIT = 2


def dot(a, b):
    return jnp.dot(a, b, preferred_element_type=F32)


def dot_t(a, b):
    return lax.dot_general(a, b, (((0,), (0,)), ((), ())), preferred_element_type=F32)


def split(a):
    high = a.astype(BF16)
    return high, (a - high.astype(F32)).astype(BF16)


def loop(low, high, body):
    def step(i, carry):
        body(i)
        return carry

    lax.fori_loop(low, high, step, 0)


def start_of_filter(gram):
    width = gram.shape[0]
    row = lax.broadcasted_iota(jnp.int32, gram.shape, 0)
    col = lax.broadcasted_iota(jnp.int32, gram.shape, 1)
    eye = row == col
    trace = jnp.sum(jnp.where(eye, gram, 0.0), axis=(0, 1), keepdims=True)
    shifted = gram * (1.0 / (trace / width)) - jnp.where(eye, 1.0, 0.0)
    norm = jnp.sqrt(jnp.sum(shifted * shifted, axis=(0, 1), keepdims=True))
    return shifted * (1.0 / (1.0 + norm))


def filter_step(iterate):
    low = iterate.astype(BF16)
    square = dot(low, low).astype(BF16)
    return 1.5 * iterate - 0.5 * dot(square, low)


def mix_of(iterate, sketch):
    return (0.5 * (sketch + dot(iterate.astype(BF16), sketch.astype(BF16)))).astype(BF16)


def projected(gram, mix):
    high, low = split(gram)
    half = dot(high, mix) + dot(low, mix)
    high, low = split(half)
    return dot_t(mix, high) + dot_t(mix, low)


def kernel(
    n_space, n_group,
    x_hbm, sk_hbm, out_ref,
    panels, other, own, sketch, diag, diag_in, diag_all,
    cs0, cr0, cg0, ca0, cs1, cr1, cg1, ca1, cs2, cr2, cg2, ca2,
    gram, gram1, it, mix0, mix1, p1, po, q, block1, block2,
    a_send, a_recv, b_send, b_recv, f_send, f_recv, l_sem,
    dr_send, dr_recv, dg_send, dg_recv, da_send, da_recv,
    r_send, r_recv, g_send, g_recv, k_send, k_recv, c_send, c_recv, z_send, z_recv,
):
    s = lax.axis_index("space")
    g = lax.axis_index("group")
    width = x_hbm.shape[1]
    block = x_hbm.shape[0] // n_group
    n_k = n_space // 2
    k = lax.div(s, 2)
    c = lax.rem(s, 2)
    gx = lax.rem(g, SPAN)
    gz = lax.div(g, SPAN)
    far = 1 - gz
    part = width // n_k
    half = width
    partner = (2 * k + 1 - c, g)

    def remote(src, dst, send, recv, to):
        return pltpu.make_async_remote_copy(
            src_ref=src, dst_ref=dst, send_sem=send, recv_sem=recv,
            device_id=to, device_id_type=MESH,
        )

    def group_peer(d):
        return s, lax.rem(g + d, n_group)

    def x_peer(d):
        return s, gz * SPAN + lax.rem(gx + d, SPAN)

    def space_peer(d):
        return lax.rem(s + d, n_space), g

    def core_peer(d):
        return 2 * lax.rem(k + d, n_k) + c, g

    def z_peer(core):
        return lax.rem(s - c + n_space // 2, n_space) + core, far * SPAN + gx

    closing = []

    def finish():
        for close in closing:
            close()

    barrier = pltpu.get_barrier_semaphore()

    def greet(to):
        pl.semaphore_signal(barrier, inc=1, device_id=to, device_id_type=MESH)

    loop(1, n_group, lambda d: greet(group_peer(d)))
    loop(1, n_space, lambda d: greet(space_peer(d)))
    loop(0, 2, lambda core: greet(z_peer(core)))

    whole = pltpu.make_async_copy(x_hbm, own, l_sem.at[0])
    whole.start()

    def block_rows(h, x):
        return pl.ds(pl.multiple_of((h * SPAN + x) * block, block), block)

    def mine(h):
        return pltpu.make_async_copy(x_hbm.at[block_rows(h, gx)], panels.at[h, gx], l_sem.at[1 + h])

    mine(0).start()
    mine(1).start()
    tests = pltpu.make_async_copy(sk_hbm, sketch, l_sem.at[3])
    tests.start()
    pl.semaphore_wait(barrier, n_group - 1 + n_space - 1 + 2)

    piece = block // PIECES

    def x_copy(d, h, at, size, send, recv):
        to = lax.rem(gx + d, SPAN)
        return remote(
            x_hbm.at[pl.ds(pl.multiple_of((h * SPAN + to) * block + at, size), size)],
            panels.at[h, gx, pl.ds(pl.multiple_of(at, size), size)],
            send, recv, (s, gz * SPAN + to))

    def first(d, p):
        return x_copy(d, far, p * piece, piece, a_send.at[d - 1, p], a_recv.at[d - 1, p])

    def second(d):
        return x_copy(d, gz, 0, block, b_send.at[d - 1], b_recv.at[d - 1])

    def send_first(j):
        p = lax.div(j, SPLIT)
        for d in (2, 1, 3):
            x_copy(d, far, j * (piece // SPLIT), piece // SPLIT,
                   a_send.at[d - 1, p], a_recv.at[d - 1, p]).start()

    def send_second(j):
        for d in (2, 1, 3):
            x_copy(d, gz, j * (piece // SPLIT), piece // SPLIT,
                   b_send.at[d - 1], b_recv.at[d - 1]).start()

    loop(0, PIECES * SPLIT, send_first)

    @closing.append
    def _():
        for d in (1, 2, 3):
            loop(0, PIECES, lambda p: first(d, p).wait_send())
            second(d).wait_send()

    def pass_rows(d, at, size):
        x = lax.rem(gx - d + SPAN, SPAN)
        rows = pl.ds(pl.multiple_of(at, size), size)
        return remote(panels.at[far, x, rows], other.at[x, rows], f_send.at[d], f_recv.at[d],
                      (s, far * SPAN + gx))

    def pass_piece(p):
        for d in (2, 1, 3):
            first(d, p).wait_recv()
            pass_rows(d, p * piece, piece).start()

    @closing.append
    def _():
        for d in range(SPAN):
            pass_rows(d, 0, block).wait_send()

    whole.wait()
    diag[...] = jnp.zeros_like(diag)

    def add_diag(j):
        rows = own[pl.ds(pl.multiple_of(j * block, block), block), :]
        diag[...] += dot_t(rows, rows)

    loop(0, n_group, add_diag)
    owner = lax.div(gx, 2)
    slot = lax.rem(gx, 2)

    def diag_copy(d):
        to = lax.rem(k + d, n_k)
        return remote(
            diag.at[pl.ds(pl.multiple_of(to * part, part), part)], diag_in.at[s],
            dr_send.at[d], dr_recv.at[s], (2 * to + owner, g))

    keeps = c == owner
    loop(1, n_k, lambda d: diag_copy(d).start())
    closing.append(lambda: loop(1, n_k, lambda d: diag_copy(d).wait_send()))

    @pl.when(jnp.logical_not(keeps))
    def _():
        diag_copy(0).start()

    mine(0).wait()
    mine(1).wait()
    pass_rows(0, 0, block).start()

    def pass_diag(d):
        return remote(diag_all.at[k, slot], diag_all.at[k, slot], dg_send.at[d], dg_recv.at[slot],
                      x_peer(d))

    @pl.when(keeps)
    def _():
        diag_in[s] = diag[pl.ds(pl.multiple_of(k * part, part), part), :]

        def arrived(d):
            at = lax.rem(s + d, n_space)
            remote(diag.at[pl.ds(0, part)], diag_in.at[at], dr_send.at[0], dr_recv.at[at],
                   (at, g)).wait_recv()

        loop(1, n_space, arrived)
        diag_all[k, slot] = jnp.sum(diag_in[...], axis=0)
        loop(1, SPAN, lambda d: pass_diag(d).start())

    @closing.append
    def _():
        @pl.when(jnp.logical_not(keeps))
        def _():
            diag_copy(0).wait_send()

        @pl.when(keeps)
        def _():
            loop(1, SPAN, lambda d: pass_diag(d).wait_send())

    loop(0, PIECES * SPLIT, send_second)
    loop(0, PIECES - 1, pass_piece)

    def diag_arrived(j):
        @pl.when(2 * c + j != gx)
        def _():
            remote(diag_all.at[k, j], diag_all.at[k, j], dg_send.at[0], dg_recv.at[j],
                   (s, gz * SPAN + 2 * c + j)).wait_recv()

    loop(0, 2, diag_arrived)

    def diag_gather(d):
        return remote(diag_all.at[k], diag_all.at[k], da_send.at[d], da_recv.at[d], core_peer(d))

    loop(1, n_k, lambda d: diag_gather(d).start())
    closing.append(lambda: loop(1, n_k, lambda d: diag_gather(d).wait_send()))

    def reduce_cross(level, cs, cr, cg, ca, all_groups, everyone, beside):
        mid, mids, mid_peer = (g, n_group, group_peer) if all_groups else (gx, SPAN, x_peer)
        at, peers, peer = (s, n_space, space_peer) if everyone else (k, n_k, core_peer)

        def scatter(d):
            to = lax.rem(s + d, n_space)
            return remote(cs.at[to], cr.at[s], r_send.at[level, d], r_recv.at[level, d], (to, g))

        def share(d):
            return remote(cg.at[mid], cg.at[mid], g_send.at[level, d], g_recv.at[level, d], mid_peer(d))

        def gather(d):
            return remote(ca.at[at], ca.at[at], k_send.at[level, d], k_recv.at[level, d], peer(d))

        loop(1, n_space, lambda d: scatter(d).start())
        cr[s] = cs[s]
        beside[0]()
        loop(1, n_space, lambda d: scatter(d).wait_recv())
        cg[mid] = jnp.sum(cr[...].astype(F32), axis=0).astype(BF16)
        loop(1, mids, lambda d: share(d).start())
        beside[1]()
        loop(1, mids, lambda d: share(d).wait_recv())
        ca[at] = jnp.sum(cg[...].astype(F32), axis=0).astype(BF16)
        loop(1, peers, lambda d: gather(d).start())
        beside[2]()
        loop(1, peers, lambda d: gather(d).wait_recv())

        @closing.append
        def _():
            loop(1, n_space, lambda d: scatter(d).wait_send())
            loop(1, mids, lambda d: share(d).wait_send())
            loop(1, peers, lambda d: gather(d).wait_send())

    tile = 256

    def mixed(a, b, mix, dst):
        upper, lower = mix[:width, :], mix[width:, :]

        def rows(j):
            here = pl.ds(pl.multiple_of(j * tile, tile), tile)
            dst[here, :] = (dot(a[here, :], upper) + dot(b[here, :], lower)).astype(BF16)

        loop(0, block // tile, rows)

    def filtered(upper, cross, lower, test, into):
        into[:width, :width] = upper
        into[width:, width:] = lower
        into[:width, width:] = cross
        into[width:, :width] = cross.T
        it[...] = start_of_filter(into[...])

        def step(_):
            it[...] = filter_step(it[...])

        loop(0, STEPS, step)
        return mix_of(it[...], test)

    def nothing():
        pass

    for d in (1, 2, 3):
        second(d).wait_recv()
    first_last = PIECES - 1
    for d in (1, 2, 3):
        first(d, first_last).wait_recv()
    for i in range(2):
        cross = dot_t(panels[0, 2 * i], panels[0, 2 * i + 1]) + dot_t(panels[1, 2 * i], panels[1, 2 * i + 1])
        cross = cross.astype(BF16).reshape(n_k, part, width)
        for kk in range(n_k):
            cs0[2 * kk + i] = cross[kk]

    def pass_last():
        for d in (2, 1, 3):
            pass_rows(d, first_last * piece, piece).start()

    reduce_cross(0, cs0, cr0, cg0, ca0, False, False, (
        pass_last, lambda: loop(1, n_k, lambda d: diag_gather(d).wait_recv()), nothing))
    tests.wait()
    mix0[0, c] = filtered(
        diag_all[:, 0].reshape(width, width), ca0[...].astype(F32).reshape(width, width),
        diag_all[:, 1].reshape(width, width), sketch[0], gram)
    swap0 = remote(mix0.at[0, c], mix0.at[0, c], c_send.at[0], c_recv.at[0], partner)
    swap0.start()
    closing.append(swap0.wait_send)

    def cross_z(n, src, dst):
        def copy(core):
            return remote(src, dst, z_send.at[n, core], z_recv.at[n, c], z_peer(core))

        def arrived(core, into):
            return remote(into, into, z_send.at[n, 0], z_recv.at[n, core], z_peer(core))

        loop(0, 2, lambda core: copy(core).start())
        closing.append(lambda: loop(0, 2, lambda core: copy(core).wait_send()))
        return arrived

    mixes = cross_z(0, mix0.at[0, c], mix0.at[1, c])

    def first_merge(pair):
        for h in range(2):
            mixed(panels.at[h, 2 * pair], panels.at[h, 2 * pair + 1], mix0.at[0, pair], p1.at[h, pair])

    first_merge(c)
    swap0.wait_recv()
    first_merge(1 - c)
    cross = dot_t(p1[0, 0], p1[0, 1]) + dot_t(p1[1, 0], p1[1, 1])
    cs1[...] = cross.astype(BF16).reshape(n_space, part // 2, width)
    swap1 = remote(block1.at[c], block1.at[c], c_send.at[1], c_recv.at[1], partner)

    def diag1():
        block1[c] = projected(gram[...], mix0[0, c])
        swap1.start()

    def other_rows():
        for core in range(2):
            mixes(core, mix0.at[1, core]).wait_recv()
        for d in range(SPAN):
            pass_rows(d, 0, block).wait_recv()
        for pair in range(2):
            mixed(other.at[2 * pair], other.at[2 * pair + 1], mix0.at[1, pair], po.at[pair])

    reduce_cross(1, cs1, cr1, cg1, ca1, False, True, (diag1, nothing, other_rows))
    swap1.wait_recv()
    closing.append(swap1.wait_send)
    mix1[0] = filtered(
        block1[0], ca1[...].astype(F32).reshape(width, width), block1[1], sketch[1], gram1)
    mine_half = pl.ds(pl.multiple_of(c * half, half), half)
    merges = cross_z(1, mix1.at[0, mine_half], mix1.at[1, mine_half])

    mixed(p1.at[gz, 0], p1.at[gz, 1], mix1.at[0], q.at[gz])
    for core in range(2):
        merges(core, mix1.at[1, pl.ds(core * half, half)]).wait_recv()
    mixed(po.at[0], po.at[1], mix1.at[1], q.at[far])
    cs2[...] = dot_t(q[0], q[1]).astype(BF16).reshape(n_space, part // 2, width)
    rows2 = pl.ds(pl.multiple_of(c * (width // 2), width // 2), width // 2)
    later = []

    def diag2():
        block2[gz] = projected(gram1[...], mix1[0])
        later.append(cross_z(2, block2.at[gz, rows2], block2.at[gz, rows2]))

    reduce_cross(2, cs2, cr2, cg2, ca2, True, True, (diag2, nothing, nothing))
    for core in range(2):
        later[0](core, block2.at[far, pl.ds(core * (width // 2), width // 2)]).wait_recv()
    last = filtered(
        block2[0], ca2[...].astype(F32).reshape(width, width), block2[1], sketch[2], gram)
    upper, lower = last[:width, :], last[width:, :]

    def rows(j):
        here = pl.ds(pl.multiple_of(j * tile, tile), tile)
        out_ref[here, :] = (dot(q[0, here, :], upper) + dot(q[1, here, :], lower)).astype(BF16)

    loop(0, block // tile, rows)
    finish()


def body(n_space, n_group, snapshot_basis, sketch):
    rows, width = snapshot_basis.shape
    block = rows // n_group
    n_k = n_space // 2
    part = width // n_k
    dma = pltpu.SemaphoreType.DMA
    vmem = pltpu.VMEM
    thin = part // 2
    scratch = [
        vmem((2, SPAN, block, width), BF16), vmem((SPAN, block, width), BF16), vmem((rows, width), BF16),
        vmem(sketch.shape, F32),
        vmem((width, width), F32), vmem((n_space, part, width), F32), vmem((n_k, 2, part, width), F32),
        vmem((n_space, part, width), BF16), vmem((n_space, part, width), BF16),
        vmem((SPAN, part, width), BF16), vmem((n_k, part, width), BF16),
        vmem((n_space, thin, width), BF16), vmem((n_space, thin, width), BF16),
        vmem((SPAN, thin, width), BF16), vmem((n_space, thin, width), BF16),
        vmem((n_space, thin, width), BF16), vmem((n_space, thin, width), BF16),
        vmem((n_group, thin, width), BF16), vmem((n_space, thin, width), BF16),
        vmem((2 * width, 2 * width), F32), vmem((2 * width, 2 * width), F32), vmem((2 * width, 2 * width), F32),
        vmem((2, 2, 2 * width, width), BF16), vmem((2, 2 * width, width), BF16),
        vmem((2, 2, block, width), BF16), vmem((2, block, width), BF16), vmem((2, block, width), BF16),
        vmem((2, width, width), F32), vmem((2, width, width), F32),
        dma((3, PIECES)), dma((3, PIECES)), dma((3,)), dma((3,)), dma((SPAN,)), dma((SPAN,)), dma((4,)),
        dma((n_k,)), dma((n_space,)), dma((SPAN,)), dma((2,)), dma((n_k,)), dma((n_k,)),
        dma((3, n_space)), dma((3, n_space)), dma((3, n_group)), dma((3, n_group)),
        dma((3, n_space)), dma((3, n_space)), dma((2,)), dma((2,)), dma((3, 2)), dma((3, 2)),
    ]
    return pl.pallas_call(
        functools.partial(kernel, n_space, n_group),
        out_shape=jax.ShapeDtypeStruct((block, width), BF16),
        in_specs=[pl.BlockSpec(memory_space=pl.ANY)] * 2,
        out_specs=pl.BlockSpec(memory_space=pltpu.VMEM),
        scratch_shapes=scratch,
        compiler_params=pltpu.CompilerParams(
            collective_id=0, has_side_effects=True, vmem_limit_bytes=56 * 1024 * 1024),
        name="merge",
    )(snapshot_basis, sketch)


def solution(mesh):
    in_specs = (P("space", "group"), P())
    out_specs = P(("space", "group"), None)
    step = functools.partial(body, mesh.shape["space"], mesh.shape["group"])
    return jax.shard_map(step, mesh=mesh, in_specs=in_specs, out_specs=out_specs, check_vma=False)
```

```python
import functools

import jax
import jax.numpy as jnp
from jax import lax
from jax.experimental import pallas as pl
from jax.experimental.pallas import tpu as pltpu
from jax.sharding import PartitionSpec as P

STEPS = 5
MESH = pl.DeviceIdType.MESH
F32 = jnp.float32
BF16 = jnp.bfloat16
SPAN = 4
PIECES = 4
SPLIT = 2
TILE = 512


def dot(a, b):
    return jnp.dot(a, b, preferred_element_type=F32)


def dot_t(a, b):
    return lax.dot_general(a, b, (((0,), (0,)), ((), ())), preferred_element_type=F32)


def split(a):
    high = a.astype(BF16)
    return high, (a - high.astype(F32)).astype(BF16)


def loop(low, high, body):
    def step(i, carry):
        body(i)
        return carry

    lax.fori_loop(low, high, step, 0)


def start_of_filter(gram):
    width = gram.shape[0]
    row = lax.broadcasted_iota(jnp.int32, gram.shape, 0)
    col = lax.broadcasted_iota(jnp.int32, gram.shape, 1)
    eye = row == col
    trace = jnp.sum(jnp.where(eye, gram, 0.0), axis=(0, 1), keepdims=True)
    shifted = gram * (1.0 / (trace / width)) - jnp.where(eye, 1.0, 0.0)
    norm = jnp.sqrt(jnp.sum(shifted * shifted, axis=(0, 1), keepdims=True))
    return shifted * (1.0 / (1.0 + norm))


def filter_step(iterate):
    low = iterate.astype(BF16)
    square = dot(low, low).astype(BF16)
    return 1.5 * iterate - 0.5 * dot(square, low)


def mix_of(iterate, sketch):
    low = iterate.astype(BF16)
    once = dot(low, sketch.astype(BF16))
    twice = dot(low, once.astype(BF16))
    thrice = dot(low, twice.astype(BF16))
    return (0.5 * (sketch + 1.5 * once - 0.5 * thrice)).astype(BF16)


def projected(gram, mix):
    high, low = split(gram)
    half = dot(high, mix) + dot(low, mix)
    high, low = split(half)
    return dot_t(mix, high) + dot_t(mix, low)


def kernel(
    n_space, n_group,
    x_hbm, sk_hbm, out_ref,
    panels, other, own, sketch, diag, diag_in, diag_all,
    cs0, cr0, cg0, ca0, cs1, cr1, cg1, ca1, cs2, cr2, cg2, ca2,
    gram, gram1, it, mix0, mix1, pf, q, block1, cross1, block2,
    a_send, a_recv, b_send, b_recv, f_send, f_recv, l_sem,
    dr_send, dr_recv, dg_send, dg_recv, da_send, da_recv,
    r_send, r_recv, g_send, g_recv, k_send, k_recv, c_send, c_recv, z_send, z_recv, e_send, e_recv,
):
    s = lax.axis_index("space")
    g = lax.axis_index("group")
    width = x_hbm.shape[1]
    block = x_hbm.shape[0] // n_group
    n_k = n_space // 2
    k = lax.div(s, 2)
    c = lax.rem(s, 2)
    gx = lax.rem(g, SPAN)
    gz = lax.div(g, SPAN)
    far = 1 - gz
    part = width // n_k
    partner = (2 * k + 1 - c, g)

    def remote(src, dst, send, recv, to):
        return pltpu.make_async_remote_copy(
            src_ref=src, dst_ref=dst, send_sem=send, recv_sem=recv,
            device_id=to, device_id_type=MESH,
        )

    def group_peer(d):
        return s, lax.rem(g + d, n_group)

    def x_peer(d):
        return s, gz * SPAN + lax.rem(gx + d, SPAN)

    def space_peer(d):
        return lax.rem(s + d, n_space), g

    def core_peer(d):
        return 2 * lax.rem(k + d, n_k) + c, g

    def z_peer(core):
        return lax.rem(s - c + n_space // 2, n_space) + core, far * SPAN + gx

    closing = []

    def finish():
        for close in closing:
            close()

    barrier = pltpu.get_barrier_semaphore()

    def greet(to):
        pl.semaphore_signal(barrier, inc=1, device_id=to, device_id_type=MESH)

    loop(1, n_group, lambda d: greet(group_peer(d)))
    loop(1, n_space, lambda d: greet(space_peer(d)))
    loop(0, 2, lambda core: greet(z_peer(core)))

    whole = pltpu.make_async_copy(x_hbm, own, l_sem.at[0])
    whole.start()

    def block_rows(h, x):
        return pl.ds(pl.multiple_of((h * SPAN + x) * block, block), block)

    def mine(h):
        return pltpu.make_async_copy(x_hbm.at[block_rows(h, gx)], panels.at[h, gx], l_sem.at[1 + h])

    mine(0).start()
    mine(1).start()
    tests = pltpu.make_async_copy(sk_hbm, sketch, l_sem.at[3])
    tests.start()
    pl.semaphore_wait(barrier, n_group - 1 + n_space - 1 + 2)

    piece = block // PIECES

    def x_copy(d, h, at, size, send, recv):
        to = lax.rem(gx + d, SPAN)
        return remote(
            x_hbm.at[pl.ds(pl.multiple_of((h * SPAN + to) * block + at, size), size)],
            panels.at[h, gx, pl.ds(pl.multiple_of(at, size), size)],
            send, recv, (s, gz * SPAN + to))

    def first(d, p):
        return x_copy(d, far, p * piece, piece, a_send.at[d - 1, p], a_recv.at[d - 1, p])

    def second(d):
        return x_copy(d, gz, 0, block, b_send.at[d - 1], b_recv.at[d - 1])

    def send_first(j):
        p = lax.div(j, SPLIT)
        for d in (2, 1, 3):
            x_copy(d, far, j * (piece // SPLIT), piece // SPLIT,
                   a_send.at[d - 1, p], a_recv.at[d - 1, p]).start()

    def send_second(j):
        for d in (2, 1, 3):
            x_copy(d, gz, j * (piece // SPLIT), piece // SPLIT,
                   b_send.at[d - 1], b_recv.at[d - 1]).start()

    loop(0, PIECES * SPLIT, send_first)

    @closing.append
    def _():
        for d in (1, 2, 3):
            loop(0, PIECES, lambda p: first(d, p).wait_send())
            second(d).wait_send()

    def pass_rows(d, at, size):
        x = lax.rem(gx - d + SPAN, SPAN)
        rows = pl.ds(pl.multiple_of(at, size), size)
        return remote(panels.at[far, x, rows], other.at[x, rows], f_send.at[d], f_recv.at[d],
                      (s, far * SPAN + gx))

    def pass_piece(p):
        for d in (2, 1, 3):
            first(d, p).wait_recv()
            pass_rows(d, p * piece, piece).start()

    @closing.append
    def _():
        for d in range(SPAN):
            pass_rows(d, 0, block).wait_send()

    whole.wait()
    diag[...] = jnp.zeros_like(diag)

    def add_diag(j):
        rows = own[pl.ds(pl.multiple_of(j * block, block), block), :]
        diag[...] += dot_t(rows, rows)

    loop(0, n_group, add_diag)
    owner = lax.div(gx, 2)
    slot = lax.rem(gx, 2)

    def diag_copy(d):
        to = lax.rem(k + d, n_k)
        return remote(
            diag.at[pl.ds(pl.multiple_of(to * part, part), part)], diag_in.at[s],
            dr_send.at[d], dr_recv.at[s], (2 * to + owner, g))

    keeps = c == owner
    loop(1, n_k, lambda d: diag_copy(d).start())
    closing.append(lambda: loop(1, n_k, lambda d: diag_copy(d).wait_send()))

    @pl.when(jnp.logical_not(keeps))
    def _():
        diag_copy(0).start()

    mine(0).wait()
    mine(1).wait()
    pass_rows(0, 0, block).start()

    def pass_diag(d):
        return remote(diag_all.at[k, slot], diag_all.at[k, slot], dg_send.at[d], dg_recv.at[slot],
                      x_peer(d))

    @pl.when(keeps)
    def _():
        diag_in[s] = diag[pl.ds(pl.multiple_of(k * part, part), part), :]

        def arrived(d):
            at = lax.rem(s + d, n_space)
            remote(diag.at[pl.ds(0, part)], diag_in.at[at], dr_send.at[0], dr_recv.at[at],
                   (at, g)).wait_recv()

        loop(1, n_space, arrived)
        diag_all[k, slot] = jnp.sum(diag_in[...], axis=0)
        loop(1, SPAN, lambda d: pass_diag(d).start())

    @closing.append
    def _():
        @pl.when(jnp.logical_not(keeps))
        def _():
            diag_copy(0).wait_send()

        @pl.when(keeps)
        def _():
            loop(1, SPAN, lambda d: pass_diag(d).wait_send())

    loop(0, PIECES * SPLIT, send_second)
    loop(0, PIECES - 1, pass_piece)

    def diag_arrived(j):
        @pl.when(2 * c + j != gx)
        def _():
            remote(diag_all.at[k, j], diag_all.at[k, j], dg_send.at[0], dg_recv.at[j],
                   (s, gz * SPAN + 2 * c + j)).wait_recv()

    loop(0, 2, diag_arrived)

    def diag_gather(d):
        return remote(diag_all.at[k], diag_all.at[k], da_send.at[d], da_recv.at[d], core_peer(d))

    loop(1, n_k, lambda d: diag_gather(d).start())
    closing.append(lambda: loop(1, n_k, lambda d: diag_gather(d).wait_send()))

    class CrossSum:
        def __init__(self, level, cs, cr, cg, ca, all_groups, everyone):
            mid, self.mids, mid_peer = (g, n_group, group_peer) if all_groups else (gx, SPAN, x_peer)
            at, self.peers, peer = (s, n_space, space_peer) if everyone else (k, n_k, core_peer)
            self.cs, self.cr, self.cg, self.ca, self.mid, self.at = cs, cr, cg, ca, mid, at

            def scatter(d):
                to = lax.rem(s + d, n_space)
                return remote(cs.at[to], cr.at[s], r_send.at[level, d], r_recv.at[level, d], (to, g))

            def share(d):
                return remote(cg.at[mid], cg.at[mid], g_send.at[level, d], g_recv.at[level, d], mid_peer(d))

            def gather(d):
                return remote(ca.at[at], ca.at[at], k_send.at[level, d], k_recv.at[level, d], peer(d))

            self.scatter, self.share, self.gather = scatter, share, gather

        def begin(self):
            loop(1, n_space, lambda d: self.scatter(d).start())
            self.cr[s] = self.cs[s]

            @closing.append
            def _():
                loop(1, n_space, lambda d: self.scatter(d).wait_send())
                loop(1, self.mids, lambda d: self.share(d).wait_send())
                loop(1, self.peers, lambda d: self.gather(d).wait_send())

        def to_share(self):
            loop(1, n_space, lambda d: self.scatter(d).wait_recv())
            self.cg[self.mid] = jnp.sum(self.cr[...].astype(F32), axis=0).astype(BF16)
            loop(1, self.mids, lambda d: self.share(d).start())

        def to_gather(self):
            loop(1, self.mids, lambda d: self.share(d).wait_recv())
            self.ca[self.at] = jnp.sum(self.cg[...].astype(F32), axis=0).astype(BF16)
            loop(1, self.peers, lambda d: self.gather(d).start())

        def end(self):
            loop(1, self.peers, lambda d: self.gather(d).wait_recv())

    def mixed(a, b, mix, dst):
        for j in range(block // TILE):
            rows = pl.ds(j * TILE, TILE)
            dst[rows, :] = (dot(a[rows, :], mix[:width, :]) + dot(b[rows, :], mix[width:, :])).astype(BF16)

    def nothing():
        pass

    def filtered(upper, cross, lower, test, into, midway=nothing):
        into[:width, :width] = upper
        into[width:, width:] = lower
        into[:width, width:] = cross
        into[width:, :width] = cross.T
        it[...] = start_of_filter(into[...])

        def step(_):
            it[...] = filter_step(it[...])

        loop(0, 2, step)
        midway()
        loop(2, STEPS - 1, step)
        return mix_of(it[...], test)

    for d in (1, 2, 3):
        second(d).wait_recv()
    first_last = PIECES - 1
    for d in (1, 2, 3):
        first(d, first_last).wait_recv()
    sum0 = CrossSum(0, cs0, cr0, cg0, ca0, False, False)
    sum1 = CrossSum(1, cs1, cr1, cg1, ca1, False, False)
    sum2 = CrossSum(2, cs2, cr2, cg2, ca2, True, True)

    def raw_cross(a, b):
        cross = dot_t(panels[0, a], panels[0, b]) + dot_t(panels[1, a], panels[1, b])
        return cross.astype(BF16).reshape(n_k, part, width)

    for i in range(2):
        cross = raw_cross(2 * i, 2 * i + 1)
        for kk in range(n_k):
            cs0[2 * kk + i] = cross[kk]
    sum0.begin()
    for i in range(2):
        for j in range(2):
            cross = raw_cross(i, 2 + j)
            for kk in range(n_k):
                cs1[2 * kk + i, j] = cross[kk]
    sum0.to_share()
    sum1.begin()
    for d in (2, 1, 3):
        pass_rows(d, first_last * piece, piece).start()
    loop(1, n_k, lambda d: diag_gather(d).wait_recv())
    sum0.to_gather()
    sum1.to_share()
    tests.wait()
    sum0.end()
    mix0[0, c] = filtered(
        diag_all[:, 0].reshape(width, width), ca0[...].astype(F32).reshape(width, width),
        diag_all[:, 1].reshape(width, width), sketch[0], gram, sum1.to_gather)
    swap0 = remote(mix0.at[0, c], mix0.at[0, c], c_send.at[0], c_recv.at[0], partner)
    swap0.start()
    mixes = remote(mix0.at[0, c], mix0.at[1, c], z_send.at[0], z_recv.at[0], z_peer(c))
    mixes.start()

    block1[c] = projected(gram[...], mix0[0, c])
    swap1 = remote(block1.at[c], block1.at[c], c_send.at[1], c_recv.at[1], partner)
    swap1.start()
    mixed(panels.at[gz, 2 * c], panels.at[gz, 2 * c + 1], mix0.at[0, c], pf.at[gz, c])
    swap0.wait_recv()
    mixed(panels.at[gz, 2 - 2 * c], panels.at[gz, 3 - 2 * c], mix0.at[0, 1 - c], pf.at[gz, 1 - c])
    sum1.end()
    raw = ca1[...]
    high, low = split(
        dot(raw[:, 0].reshape(width, width), mix0[0, 1, :width, :])
        + dot(raw[:, 1].reshape(width, width), mix0[0, 1, width:, :]))
    left = mix0[0, 0, pl.ds(pl.multiple_of(c * width, width), width), :]
    cross1[c] = dot_t(left, high) + dot_t(left, low)
    swap2 = remote(cross1.at[c], cross1.at[c], c_send.at[2], c_recv.at[2], partner)
    swap2.start()
    swap1.wait_recv()
    swap2.wait_recv()
    mix1[0] = filtered(block1[0], cross1[0] + cross1[1], block1[1], sketch[1], gram1)
    my_half = pl.ds(pl.multiple_of(c * width, width), width)
    merges = remote(mix1.at[0, my_half], mix1.at[1, my_half], z_send.at[1], z_recv.at[1], z_peer(c))
    merges.start()
    mixes.wait_recv()
    swap3 = remote(mix0.at[1, c], mix0.at[1, c], c_send.at[3], c_recv.at[3], partner)
    swap3.start()

    mixed(pf.at[gz, 0], pf.at[gz, 1], mix1.at[0], q.at[gz])
    for d in range(SPAN):
        pass_rows(d, 0, block).wait_recv()
    mixed(other.at[2 * c], other.at[2 * c + 1], mix0.at[1, c], pf.at[far, c])
    swap3.wait_recv()
    mixed(other.at[2 - 2 * c], other.at[3 - 2 * c], mix0.at[1, 1 - c], pf.at[far, 1 - c])
    merges.wait_recv()
    swap4 = remote(mix1.at[1, my_half], mix1.at[1, my_half], c_send.at[4], c_recv.at[4], partner)
    swap4.start()
    swap4.wait_recv()
    mixed(pf.at[far, 0], pf.at[far, 1], mix1.at[1], q.at[far])

    @closing.append
    def _():
        for copy in (swap0, swap1, swap2, swap3, swap4, mixes, merges):
            copy.wait_send()

    cs2[...] = dot_t(q[0], q[1]).astype(BF16).reshape(n_space, part // 2, width)
    sum2.begin()
    block2[gz] = projected(gram1[...], mix1[0])
    strip = width // 2

    def strip_copy(core):
        rows = pl.ds(pl.multiple_of(c * strip, strip), strip)
        return remote(block2.at[gz, rows], block2.at[gz, rows], e_send.at[core], e_recv.at[c], z_peer(core))

    def strip_arrived(core):
        rows = pl.ds(pl.multiple_of(core * strip, strip), strip)
        return remote(block2.at[far, rows], block2.at[far, rows], e_send.at[0], e_recv.at[core], z_peer(core))

    loop(0, 2, lambda core: strip_copy(core).start())
    closing.append(lambda: loop(0, 2, lambda core: strip_copy(core).wait_send()))
    sum2.to_share()
    sum2.to_gather()
    loop(0, 2, lambda core: strip_arrived(core).wait_recv())
    sum2.end()
    last = filtered(
        block2[0], ca2[...].astype(F32).reshape(width, width), block2[1], sketch[2], gram)
    upper, lower = last[:width, :], last[width:, :]
    for j in range(block // TILE):
        rows = pl.ds(j * TILE, TILE)
        out_ref[rows, :] = (dot(q[0, rows, :], upper) + dot(q[1, rows, :], lower)).astype(BF16)
    finish()


def body(n_space, n_group, snapshot_basis, sketch):
    rows, width = snapshot_basis.shape
    block = rows // n_group
    n_k = n_space // 2
    part = width // n_k
    dma = pltpu.SemaphoreType.DMA
    vmem = pltpu.VMEM
    thin = part // 2
    scratch = [
        vmem((2, SPAN, block, width), BF16), vmem((SPAN, block, width), BF16), vmem((rows, width), BF16),
        vmem(sketch.shape, F32),
        vmem((width, width), F32), vmem((n_space, part, width), F32), vmem((n_k, 2, part, width), F32),
        vmem((n_space, part, width), BF16), vmem((n_space, part, width), BF16),
        vmem((SPAN, part, width), BF16), vmem((n_k, part, width), BF16),
        vmem((n_space, 2, part, width), BF16), vmem((n_space, 2, part, width), BF16),
        vmem((SPAN, 2, part, width), BF16), vmem((n_k, 2, part, width), BF16),
        vmem((n_space, thin, width), BF16), vmem((n_space, thin, width), BF16),
        vmem((n_group, thin, width), BF16), vmem((n_space, thin, width), BF16),
        vmem((2 * width, 2 * width), F32), vmem((2 * width, 2 * width), F32), vmem((2 * width, 2 * width), F32),
        vmem((2, 2, 2 * width, width), BF16), vmem((2, 2 * width, width), BF16),
        vmem((2, 2, block, width), BF16), vmem((2, block, width), BF16),
        vmem((2, width, width), F32), vmem((2, width, width), F32), vmem((2, width, width), F32),
        dma((3, PIECES)), dma((3, PIECES)), dma((3,)), dma((3,)), dma((SPAN,)), dma((SPAN,)), dma((4,)),
        dma((n_k,)), dma((n_space,)), dma((SPAN,)), dma((2,)), dma((n_k,)), dma((n_k,)),
        dma((3, n_space)), dma((3, n_space)), dma((3, n_group)), dma((3, n_group)),
        dma((3, n_space)), dma((3, n_space)), dma((5,)), dma((5,)), dma((2,)), dma((2,)), dma((2,)), dma((2,)),
    ]
    return pl.pallas_call(
        functools.partial(kernel, n_space, n_group),
        out_shape=jax.ShapeDtypeStruct((block, width), BF16),
        in_specs=[pl.BlockSpec(memory_space=pl.ANY)] * 2,
        out_specs=pl.BlockSpec(memory_space=pltpu.VMEM),
        scratch_shapes=scratch,
        compiler_params=pltpu.CompilerParams(
            collective_id=0, has_side_effects=True, vmem_limit_bytes=56 * 1024 * 1024),
        name="merge",
    )(snapshot_basis, sketch)


def solution(mesh):
    in_specs = (P("space", "group"), P())
    out_specs = P(("space", "group"), None)
    step = functools.partial(body, mesh.shape["space"], mesh.shape["group"])
    return jax.shard_map(step, mesh=mesh, in_specs=in_specs, out_specs=out_specs, check_vma=False)
```

```python
import functools

import jax
import jax.numpy as jnp
from jax import lax
from jax.experimental import pallas as pl
from jax.experimental.pallas import tpu as pltpu
from jax.sharding import PartitionSpec as P

STEPS = 5
MESH = pl.DeviceIdType.MESH
F32 = jnp.float32
BF16 = jnp.bfloat16
SPAN = 4
PIECES = 8
SPLIT = 1
TILE = 512


def dot(a, b):
    return jnp.dot(a, b, preferred_element_type=F32)


def dot_t(a, b):
    return lax.dot_general(a, b, (((0,), (0,)), ((), ())), preferred_element_type=F32)


def split(a):
    high = a.astype(BF16)
    return high, (a - high.astype(F32)).astype(BF16)


def loop(low, high, body):
    def step(i, carry):
        body(i)
        return carry

    lax.fori_loop(low, high, step, 0)


def total(a):
    return jnp.sum(a, axis=(0, 1), keepdims=True)


def diagonal_of_filter(upper, lower, into):
    width = upper.shape[0]
    row = lax.broadcasted_iota(jnp.int32, upper.shape, 0)
    col = lax.broadcasted_iota(jnp.int32, upper.shape, 1)
    eye = row == col
    scale = 1.0 / (total(jnp.where(eye, upper + lower, 0.0)) / (2 * width))
    one = jnp.where(eye, 1.0, 0.0)
    upper = upper * scale - one
    lower = lower * scale - one
    into[:width, :width] = upper
    into[width:, width:] = lower
    return scale, total(upper * upper + lower * lower)


def start_of_filter(scale, squares, cross, into):
    width = cross.shape[0]
    cross = cross * scale
    factor = 1.0 / (1.0 + jnp.sqrt(squares + 2.0 * total(cross * cross)))
    cross = cross * factor
    into[:width, width:] = cross
    into[width:, :width] = cross.T
    into[:width, :width] = into[:width, :width] * factor
    into[width:, width:] = into[width:, width:] * factor


def filter_step(iterate):
    low = iterate.astype(BF16)
    square = dot(low, low).astype(BF16)
    return 1.5 * iterate - 0.5 * dot(square, low)


def mix_of(iterate, sketch):
    low = iterate.astype(BF16)
    once = dot(low, sketch.astype(BF16))
    twice = dot(low, once.astype(BF16))
    thrice = dot(low, twice.astype(BF16))
    return (0.5 * (sketch + 1.5 * once - 0.5 * thrice)).astype(BF16)


def projected(gram, mix):
    high, low = split(gram)
    half = dot(high, mix) + dot(low, mix)
    high, low = split(half)
    return dot_t(mix, high) + dot_t(mix, low)


def kernel(
    n_space, n_group,
    x_hbm, sk_hbm, out_ref,
    panels, other, own, sketch, diag, diag_in, diag_all,
    cs0, cr0, cg0, ca0, cs1, cr1, cg1, ca1, cs2, cr2, cg2, ca2,
    gram, gram1, it, mix0, mix1, pf, q, block1, cross1, block2,
    a_send, a_recv, b_send, b_recv, f_send, f_recv, l_sem,
    dr_send, dr_recv, dg_send, dg_recv, da_send, da_recv,
    r_send, r_recv, g_send, g_recv, k_send, k_recv, c_send, c_recv, z_send, z_recv, e_send, e_recv,
):
    s = lax.axis_index("space")
    g = lax.axis_index("group")
    width = x_hbm.shape[1]
    block = x_hbm.shape[0] // n_group
    n_k = n_space // 2
    k = lax.div(s, 2)
    c = lax.rem(s, 2)
    gx = lax.rem(g, SPAN)
    gz = lax.div(g, SPAN)
    far = 1 - gz
    part = width // n_k
    partner = (2 * k + 1 - c, g)

    def remote(src, dst, send, recv, to):
        return pltpu.make_async_remote_copy(
            src_ref=src, dst_ref=dst, send_sem=send, recv_sem=recv,
            device_id=to, device_id_type=MESH,
        )

    def group_peer(d):
        return s, lax.rem(g + d, n_group)

    def x_peer(d):
        return s, gz * SPAN + lax.rem(gx + d, SPAN)

    def space_peer(d):
        return lax.rem(s + d, n_space), g

    def core_peer(d):
        return 2 * lax.rem(k + d, n_k) + c, g

    def z_peer(core):
        return lax.rem(s - c + n_space // 2, n_space) + core, far * SPAN + gx

    closing = []

    def finish():
        for close in closing:
            close()

    barrier = pltpu.get_barrier_semaphore()

    def greet(to):
        pl.semaphore_signal(barrier, inc=1, device_id=to, device_id_type=MESH)

    loop(1, n_group, lambda d: greet(group_peer(d)))
    loop(1, n_space, lambda d: greet(space_peer(d)))
    loop(0, 2, lambda core: greet(z_peer(core)))

    whole = pltpu.make_async_copy(x_hbm, own, l_sem.at[0])
    whole.start()

    def block_rows(h, x):
        return pl.ds(pl.multiple_of((h * SPAN + x) * block, block), block)

    def mine(h):
        return pltpu.make_async_copy(x_hbm.at[block_rows(h, gx)], panels.at[h, gx], l_sem.at[1 + h])

    mine(0).start()
    mine(1).start()
    tests = pltpu.make_async_copy(sk_hbm, sketch, l_sem.at[3])
    tests.start()
    pl.semaphore_wait(barrier, n_group - 1 + n_space - 1 + 2)

    piece = block // PIECES

    def x_copy(d, h, at, size, send, recv):
        to = lax.rem(gx + d, SPAN)
        return remote(
            own.at[pl.ds(pl.multiple_of((h * SPAN + to) * block + at, size), size)],
            panels.at[h, gx, pl.ds(pl.multiple_of(at, size), size)],
            send, recv, (s, gz * SPAN + to))

    def first(d, p):
        return x_copy(d, far, p * piece, piece, a_send.at[d - 1, p], a_recv.at[d - 1, p])

    def second(d):
        return x_copy(d, gz, 0, block, b_send.at[d - 1], b_recv.at[d - 1])

    def send_first(j):
        p = lax.div(j, SPLIT)
        for d in (2, 1, 3):
            x_copy(d, far, j * (piece // SPLIT), piece // SPLIT,
                   a_send.at[d - 1, p], a_recv.at[d - 1, p]).start()

    def send_second(j):
        for d in (2, 1, 3):
            x_copy(d, gz, j * (piece // SPLIT), piece // SPLIT,
                   b_send.at[d - 1], b_recv.at[d - 1]).start()

    whole.wait()
    loop(0, PIECES * SPLIT, send_first)

    @closing.append
    def _():
        for d in (1, 2, 3):
            loop(0, PIECES, lambda p: first(d, p).wait_send())
            second(d).wait_send()

    def pass_rows(d, at, size):
        x = lax.rem(gx - d + SPAN, SPAN)
        rows = pl.ds(pl.multiple_of(at, size), size)
        return remote(panels.at[far, x, rows], other.at[x, rows], f_send.at[d], f_recv.at[d],
                      (s, far * SPAN + gx))

    def pass_piece(p):
        for d in (2, 1, 3):
            first(d, p).wait_recv()
            pass_rows(d, p * piece, piece).start()

    def pass_own(at, size):
        rows = pl.ds(pl.multiple_of((far * SPAN + gx) * block + at, size), size)
        remote(own.at[rows], other.at[gx, pl.ds(at, size)], f_send.at[0], f_recv.at[0],
               (s, far * SPAN + gx)).start()

    pass_own(0, block // 2)

    @closing.append
    def _():
        for d in range(SPAN):
            pass_rows(d, 0, block).wait_send()

    diag[...] = jnp.zeros_like(diag)

    def add_diag(j):
        rows = own[pl.ds(pl.multiple_of(j * block, block), block), :]
        diag[...] += dot_t(rows, rows)

    loop(0, n_group, add_diag)
    owner = lax.div(gx, 2)
    slot = lax.rem(gx, 2)

    def diag_copy(d):
        to = lax.rem(k + d, n_k)
        return remote(
            diag.at[pl.ds(pl.multiple_of(to * part, part), part)], diag_in.at[s],
            dr_send.at[d], dr_recv.at[s], (2 * to + owner, g))

    keeps = c == owner
    loop(1, n_k, lambda d: diag_copy(d).start())
    closing.append(lambda: loop(1, n_k, lambda d: diag_copy(d).wait_send()))

    @pl.when(jnp.logical_not(keeps))
    def _():
        diag_copy(0).start()

    mine(0).wait()
    mine(1).wait()
    pass_own(block // 2, block // 2)

    def pass_diag(d):
        return remote(diag_all.at[k, slot], diag_all.at[k, slot], dg_send.at[d], dg_recv.at[slot],
                      x_peer(d))

    @pl.when(keeps)
    def _():
        diag_in[s] = diag[pl.ds(pl.multiple_of(k * part, part), part), :]

        def arrived(d):
            at = lax.rem(s + d, n_space)
            remote(diag.at[pl.ds(0, part)], diag_in.at[at], dr_send.at[0], dr_recv.at[at],
                   (at, g)).wait_recv()

        loop(1, n_space, arrived)
        diag_all[k, slot] = jnp.sum(diag_in[...], axis=0)
        loop(1, SPAN, lambda d: pass_diag(d).start())

    @closing.append
    def _():
        @pl.when(jnp.logical_not(keeps))
        def _():
            diag_copy(0).wait_send()

        @pl.when(keeps)
        def _():
            loop(1, SPAN, lambda d: pass_diag(d).wait_send())

    loop(0, PIECES * SPLIT, send_second)
    loop(0, PIECES - 2, pass_piece)

    def diag_arrived(j):
        @pl.when(2 * c + j != gx)
        def _():
            remote(diag_all.at[k, j], diag_all.at[k, j], dg_send.at[0], dg_recv.at[j],
                   (s, gz * SPAN + 2 * c + j)).wait_recv()

    loop(0, 2, diag_arrived)

    def diag_gather(d):
        return remote(diag_all.at[k], diag_all.at[k], da_send.at[d], da_recv.at[d], core_peer(d))

    loop(1, n_k, lambda d: diag_gather(d).start())
    closing.append(lambda: loop(1, n_k, lambda d: diag_gather(d).wait_send()))
    pass_piece(PIECES - 2)

    class CrossSum:
        def __init__(self, level, cs, cr, cg, ca, all_groups, everyone):
            mid, self.mids, mid_peer = (g, n_group, group_peer) if all_groups else (gx, SPAN, x_peer)
            at, self.peers, peer = (s, n_space, space_peer) if everyone else (k, n_k, core_peer)
            self.cs, self.cr, self.cg, self.ca, self.mid, self.at = cs, cr, cg, ca, mid, at

            def scatter(d):
                to = lax.rem(s + d, n_space)
                return remote(cs.at[to], cr.at[s], r_send.at[level, d], r_recv.at[level, d], (to, g))

            def share(d):
                return remote(cg.at[mid], cg.at[mid], g_send.at[level, d], g_recv.at[level, d], mid_peer(d))

            def gather(d):
                return remote(ca.at[at], ca.at[at], k_send.at[level, d], k_recv.at[level, d], peer(d))

            self.scatter, self.share, self.gather = scatter, share, gather

        def begin(self):
            loop(1, n_space, lambda d: self.scatter(d).start())
            self.cr[s] = self.cs[s]

            @closing.append
            def _():
                loop(1, n_space, lambda d: self.scatter(d).wait_send())
                loop(1, self.mids, lambda d: self.share(d).wait_send())
                loop(1, self.peers, lambda d: self.gather(d).wait_send())

        def to_share(self):
            loop(1, n_space, lambda d: self.scatter(d).wait_recv())
            self.cg[self.mid] = jnp.sum(self.cr[...].astype(F32), axis=0).astype(BF16)
            loop(1, self.mids, lambda d: self.share(d).start())

        def to_gather(self):
            loop(1, self.mids, lambda d: self.share(d).wait_recv())
            self.ca[self.at] = jnp.sum(self.cg[...].astype(F32), axis=0).astype(BF16)
            loop(1, self.peers, lambda d: self.gather(d).start())

        def end(self):
            loop(1, self.peers, lambda d: self.gather(d).wait_recv())

    def mixed(a, b, mix, dst):
        for j in range(block // TILE):
            rows = pl.ds(j * TILE, TILE)
            dst[rows, :] = (dot(a[rows, :], mix[:width, :]) + dot(b[rows, :], mix[width:, :])).astype(BF16)

    def nothing():
        pass

    def filtered(scale, squares, cross, test, midway=nothing):
        start_of_filter(scale, squares, cross, it)

        def step(_):
            it[...] = filter_step(it[...])

        loop(0, 2, step)
        midway()
        loop(2, STEPS - 1, step)
        return mix_of(it[...], test)

    def keep(into, upper, cross, lower):
        into[:width, :width] = upper
        into[width:, width:] = lower
        into[:width, width:] = cross
        into[width:, :width] = cross.T

    for d in (1, 2, 3):
        second(d).wait_recv()
    first_last = PIECES - 1
    for d in (1, 2, 3):
        first(d, first_last).wait_recv()
    sum0 = CrossSum(0, cs0, cr0, cg0, ca0, False, False)
    sum1 = CrossSum(1, cs1, cr1, cg1, ca1, False, False)
    sum2 = CrossSum(2, cs2, cr2, cg2, ca2, True, True)

    def raw_cross(a, b):
        cross = dot_t(panels[0, a], panels[0, b]) + dot_t(panels[1, a], panels[1, b])
        return cross.astype(BF16).reshape(n_k, part, width)

    for i in range(2):
        cross = raw_cross(2 * i, 2 * i + 1)
        for kk in range(n_k):
            cs0[2 * kk + i] = cross[kk]
    sum0.begin()
    for i in range(2):
        for j in range(2):
            cross = raw_cross(i, 2 + j)
            for kk in range(n_k):
                cs1[2 * kk + i, j] = cross[kk]
    sum1.begin()
    sum0.to_share()
    loop(1, n_k, lambda d: diag_gather(d).wait_recv())
    sum0.to_gather()
    for d in (2, 1, 3):
        pass_rows(d, first_last * piece, piece).start()
    sum1.to_share()
    tests.wait()
    upper, lower = (diag_all[:, j].reshape(width, width) for j in range(2))
    scale, squares = diagonal_of_filter(upper, lower, it)
    sum0.end()

    cross = ca0[...].astype(F32).reshape(width, width)
    mix0[0, c] = filtered(scale, squares, cross, sketch[0], sum1.to_gather)
    swap0 = remote(mix0.at[0, c], mix0.at[0, c], c_send.at[0], c_recv.at[0], partner)
    swap0.start()
    mixes = remote(mix0.at[0, c], mix0.at[1, c], z_send.at[0], z_recv.at[0], z_peer(c))
    mixes.start()

    keep(gram, *(diag_all[:, 0].reshape(width, width), ca0[...].astype(F32).reshape(width, width),
                 diag_all[:, 1].reshape(width, width)))
    block1[c] = projected(gram[...], mix0[0, c])
    swap1 = remote(block1.at[c], block1.at[c], c_send.at[1], c_recv.at[1], partner)
    swap1.start()
    mixed(panels.at[gz, 2 * c], panels.at[gz, 2 * c + 1], mix0.at[0, c], pf.at[gz, c])
    swap0.wait_recv()
    mixed(panels.at[gz, 2 - 2 * c], panels.at[gz, 3 - 2 * c], mix0.at[0, 1 - c], pf.at[gz, 1 - c])
    swap1.wait_recv()
    scale, squares = diagonal_of_filter(block1[0], block1[1], it)
    sum1.end()
    raw = ca1[...]
    high, low = split(
        dot(raw[:, 0].reshape(width, width), mix0[0, 1, :width, :])
        + dot(raw[:, 1].reshape(width, width), mix0[0, 1, width:, :]))
    left = mix0[0, 0, pl.ds(pl.multiple_of(c * width, width), width), :]
    cross1[c] = dot_t(left, high) + dot_t(left, low)
    swap2 = remote(cross1.at[c], cross1.at[c], c_send.at[2], c_recv.at[2], partner)
    swap2.start()
    swap2.wait_recv()
    mix1[0] = filtered(scale, squares, cross1[0] + cross1[1], sketch[1])
    my_half = pl.ds(pl.multiple_of(c * width, width), width)
    merges = remote(mix1.at[0, my_half], mix1.at[1, my_half], z_send.at[1], z_recv.at[1], z_peer(c))
    merges.start()
    keep(gram1, block1[0], cross1[0] + cross1[1], block1[1])
    block2[gz] = projected(gram1[...], mix1[0])
    strip = pl.ds(pl.multiple_of(c * (width // 2), width // 2), width // 2)
    strips = remote(block2.at[gz, strip], block2.at[gz, strip], e_send.at[0], e_recv.at[0], z_peer(c))
    strips.start()
    mixes.wait_recv()
    swap3 = remote(mix0.at[1, c], mix0.at[1, c], c_send.at[3], c_recv.at[3], partner)
    swap3.start()

    mixed(pf.at[gz, 0], pf.at[gz, 1], mix1.at[0], q.at[gz])
    for d in range(SPAN):
        pass_rows(d, 0, block).wait_recv()
    mixed(other.at[2 * c], other.at[2 * c + 1], mix0.at[1, c], pf.at[far, c])
    swap3.wait_recv()
    mixed(other.at[2 - 2 * c], other.at[3 - 2 * c], mix0.at[1, 1 - c], pf.at[far, 1 - c])
    merges.wait_recv()
    swap4 = remote(mix1.at[1, my_half], mix1.at[1, my_half], c_send.at[4], c_recv.at[4], partner)
    swap4.start()
    swap4.wait_recv()
    mixed(pf.at[far, 0], pf.at[far, 1], mix1.at[1], q.at[far])

    @closing.append
    def _():
        for copy in (swap0, swap1, swap2, swap3, swap4, mixes, merges, strips):
            copy.wait_send()

    cs2[...] = dot_t(q[0], q[1]).astype(BF16).reshape(n_space, part // 2, width)
    sum2.begin()
    remote(block2.at[far, strip], block2.at[far, strip], e_send.at[0], e_recv.at[0], z_peer(c)).wait_recv()
    swap5 = remote(block2.at[far, strip], block2.at[far, strip], e_send.at[1], e_recv.at[1], partner)
    swap5.start()
    closing.append(swap5.wait_send)
    sum2.to_share()
    sum2.to_gather()
    swap5.wait_recv()
    scale, squares = diagonal_of_filter(block2[0], block2[1], it)
    sum2.end()
    last = filtered(scale, squares, ca2[...].astype(F32).reshape(width, width), sketch[2])
    upper, lower = last[:width, :], last[width:, :]
    for j in range(block // TILE):
        rows = pl.ds(j * TILE, TILE)
        out_ref[rows, :] = (dot(q[0, rows, :], upper) + dot(q[1, rows, :], lower)).astype(BF16)
    finish()


def body(n_space, n_group, snapshot_basis, sketch):
    rows, width = snapshot_basis.shape
    block = rows // n_group
    n_k = n_space // 2
    part = width // n_k
    dma = pltpu.SemaphoreType.DMA
    vmem = pltpu.VMEM
    thin = part // 2
    scratch = [
        vmem((2, SPAN, block, width), BF16), vmem((SPAN, block, width), BF16), vmem((rows, width), BF16),
        vmem(sketch.shape, F32),
        vmem((width, width), F32), vmem((n_space, part, width), F32), vmem((n_k, 2, part, width), F32),
        vmem((n_space, part, width), BF16), vmem((n_space, part, width), BF16),
        vmem((SPAN, part, width), BF16), vmem((n_k, part, width), BF16),
        vmem((n_space, 2, part, width), BF16), vmem((n_space, 2, part, width), BF16),
        vmem((SPAN, 2, part, width), BF16), vmem((n_k, 2, part, width), BF16),
        vmem((n_space, thin, width), BF16), vmem((n_space, thin, width), BF16),
        vmem((n_group, thin, width), BF16), vmem((n_space, thin, width), BF16),
        vmem((2 * width, 2 * width), F32), vmem((2 * width, 2 * width), F32), vmem((2 * width, 2 * width), F32),
        vmem((2, 2, 2 * width, width), BF16), vmem((2, 2 * width, width), BF16),
        vmem((2, 2, block, width), BF16), vmem((2, block, width), BF16),
        vmem((2, width, width), F32), vmem((2, width, width), F32), vmem((2, width, width), F32),
        dma((3, PIECES)), dma((3, PIECES)), dma((3,)), dma((3,)), dma((SPAN,)), dma((SPAN,)), dma((4,)),
        dma((n_k,)), dma((n_space,)), dma((SPAN,)), dma((2,)), dma((n_k,)), dma((n_k,)),
        dma((3, n_space)), dma((3, n_space)), dma((3, n_group)), dma((3, n_group)),
        dma((3, n_space)), dma((3, n_space)), dma((5,)), dma((5,)), dma((2,)), dma((2,)), dma((2,)), dma((2,)),
    ]
    return pl.pallas_call(
        functools.partial(kernel, n_space, n_group),
        out_shape=jax.ShapeDtypeStruct((block, width), BF16),
        in_specs=[pl.BlockSpec(memory_space=pl.ANY)] * 2,
        out_specs=pl.BlockSpec(memory_space=pltpu.VMEM),
        scratch_shapes=scratch,
        compiler_params=pltpu.CompilerParams(
            collective_id=0, has_side_effects=True, vmem_limit_bytes=56 * 1024 * 1024),
        name="merge",
    )(snapshot_basis, sketch)


def solution(mesh):
    in_specs = (P("space", "group"), P())
    out_specs = P(("space", "group"), None)
    step = functools.partial(body, mesh.shape["space"], mesh.shape["group"])
    return jax.shard_map(step, mesh=mesh, in_specs=in_specs, out_specs=out_specs, check_vma=False)
```

```python
import functools

import jax
import jax.numpy as jnp
from jax import lax
from jax.experimental import pallas as pl
from jax.experimental.pallas import tpu as pltpu
from jax.sharding import PartitionSpec as P

STEPS = 5
MESH = pl.DeviceIdType.MESH
F32 = jnp.float32
BF16 = jnp.bfloat16
SPAN = 4
PIECES = 8
SPLIT = 1
TILE = 512


def dot(a, b):
    return jnp.dot(a, b, preferred_element_type=F32)


def dot_t(a, b):
    return lax.dot_general(a, b, (((0,), (0,)), ((), ())), preferred_element_type=F32)


def split(a):
    high = a.astype(BF16)
    return high, (a - high.astype(F32)).astype(BF16)


def loop(low, high, body):
    def step(i, carry):
        body(i)
        return carry

    lax.fori_loop(low, high, step, 0)


def total(a):
    return jnp.sum(a, axis=(0, 1), keepdims=True)


def diagonal_of_filter(upper, lower, into):
    width = upper.shape[0]
    row = lax.broadcasted_iota(jnp.int32, upper.shape, 0)
    col = lax.broadcasted_iota(jnp.int32, upper.shape, 1)
    eye = row == col
    scale = 1.0 / (total(jnp.where(eye, upper + lower, 0.0)) / (2 * width))
    one = jnp.where(eye, 1.0, 0.0)
    upper = upper * scale - one
    lower = lower * scale - one
    into[:width, :width] = upper
    into[width:, width:] = lower
    return scale, total(upper * upper + lower * lower)


def start_of_filter(scale, squares, cross, into):
    width = cross.shape[0]
    cross = cross * scale
    factor = 1.0 / (1.0 + jnp.sqrt(squares + 2.0 * total(cross * cross)))
    cross = cross * factor
    into[:width, width:] = cross
    into[width:, :width] = cross.T
    into[:width, :width] = into[:width, :width] * factor
    into[width:, width:] = into[width:, width:] * factor


def filter_step(iterate, low, square):
    width = iterate.shape[0] // 2
    a, b = pl.ds(0, width), pl.ds(width, width)
    low[...] = iterate[...].astype(BF16)
    square[a, :] = dot(low[a, :], low[...]).astype(BF16)
    square[b, b] = dot(low[b, :], low[:, b]).astype(BF16)
    square[b, a] = square[a, b].T
    top = dot(square[a, :], low[...])
    corner = dot(square[b, :], low[:, b])
    iterate[a, :] = 1.5 * iterate[a, :] - 0.5 * top
    iterate[b, b] = 1.5 * iterate[b, b] - 0.5 * corner
    iterate[b, a] = iterate[a, b].T


def mix_of(iterate, sketch):
    low = iterate.astype(BF16)
    once = dot(low, sketch.astype(BF16))
    twice = dot(low, once.astype(BF16))
    thrice = dot(low, twice.astype(BF16))
    return (0.5 * (sketch + 1.5 * once - 0.5 * thrice)).astype(BF16)


def projected(gram, mix):
    high, low = split(gram)
    half = dot(high, mix) + dot(low, mix)
    high, low = split(half)
    return dot_t(mix, high) + dot_t(mix, low)


def kernel(
    n_space, n_group,
    x_hbm, sk_hbm, out_ref,
    panels, other, own, sketch, diag, diag_in, diag_all,
    cs0, cr0, cg0, ca0, cs1, cr1, cg1, ca1, cs2, cr2, cg2, ca2,
    gram, gram1, it, low, square, mix0, mix1, pf, q, block1, cross1, block2,
    a_send, a_recv, b_send, b_recv, f_send, f_recv, l_sem,
    dr_send, dr_recv, dg_send, dg_recv, da_send, da_recv,
    r_send, r_recv, g_send, g_recv, k_send, k_recv, c_send, c_recv, z_send, z_recv, e_send, e_recv,
):
    s = lax.axis_index("space")
    g = lax.axis_index("group")
    width = x_hbm.shape[1]
    block = x_hbm.shape[0] // n_group
    n_k = n_space // 2
    k = lax.div(s, 2)
    c = lax.rem(s, 2)
    gx = lax.rem(g, SPAN)
    gz = lax.div(g, SPAN)
    far = 1 - gz
    part = width // n_k
    partner = (2 * k + 1 - c, g)

    def remote(src, dst, send, recv, to):
        return pltpu.make_async_remote_copy(
            src_ref=src, dst_ref=dst, send_sem=send, recv_sem=recv,
            device_id=to, device_id_type=MESH,
        )

    def group_peer(d):
        return s, lax.rem(g + d, n_group)

    def x_peer(d):
        return s, gz * SPAN + lax.rem(gx + d, SPAN)

    def space_peer(d):
        return lax.rem(s + d, n_space), g

    def core_peer(d):
        return 2 * lax.rem(k + d, n_k) + c, g

    def z_peer(core):
        return lax.rem(s - c + n_space // 2, n_space) + core, far * SPAN + gx

    closing = []

    def finish():
        for close in closing:
            close()

    barrier = pltpu.get_barrier_semaphore()

    def greet(to):
        pl.semaphore_signal(barrier, inc=1, device_id=to, device_id_type=MESH)

    loop(1, n_group, lambda d: greet(group_peer(d)))
    loop(1, n_space, lambda d: greet(space_peer(d)))
    loop(0, 2, lambda core: greet(z_peer(core)))

    whole = pltpu.make_async_copy(x_hbm, own, l_sem.at[0])
    whole.start()

    def block_rows(h, x):
        return pl.ds(pl.multiple_of((h * SPAN + x) * block, block), block)

    def mine(h):
        return pltpu.make_async_copy(x_hbm.at[block_rows(h, gx)], panels.at[h, gx], l_sem.at[1 + h])

    mine(0).start()
    mine(1).start()
    tests = pltpu.make_async_copy(sk_hbm, sketch, l_sem.at[3])
    tests.start()
    pl.semaphore_wait(barrier, n_group - 1 + n_space - 1 + 2)

    piece = block // PIECES

    def x_copy(d, h, at, size, send, recv):
        to = lax.rem(gx + d, SPAN)
        return remote(
            own.at[pl.ds(pl.multiple_of((h * SPAN + to) * block + at, size), size)],
            panels.at[h, gx, pl.ds(pl.multiple_of(at, size), size)],
            send, recv, (s, gz * SPAN + to))

    def first(d, p):
        return x_copy(d, far, p * piece, piece, a_send.at[d - 1, p], a_recv.at[d - 1, p])

    def second(d):
        return x_copy(d, gz, 0, block, b_send.at[d - 1], b_recv.at[d - 1])

    def send_first(j):
        p = lax.div(j, SPLIT)
        for d in (2, 1, 3):
            x_copy(d, far, j * (piece // SPLIT), piece // SPLIT,
                   a_send.at[d - 1, p], a_recv.at[d - 1, p]).start()

    def send_second(j):
        for d in (2, 1, 3):
            x_copy(d, gz, j * (piece // SPLIT), piece // SPLIT,
                   b_send.at[d - 1], b_recv.at[d - 1]).start()

    whole.wait()
    loop(0, PIECES * SPLIT, send_first)

    @closing.append
    def _():
        for d in (1, 2, 3):
            loop(0, PIECES, lambda p: first(d, p).wait_send())
            second(d).wait_send()

    def pass_rows(d, at, size):
        x = lax.rem(gx - d + SPAN, SPAN)
        rows = pl.ds(pl.multiple_of(at, size), size)
        return remote(panels.at[far, x, rows], other.at[x, rows], f_send.at[d], f_recv.at[d],
                      (s, far * SPAN + gx))

    def pass_piece(p):
        for d in (2, 1, 3):
            first(d, p).wait_recv()
            pass_rows(d, p * piece, piece).start()

    def pass_own(at, size):
        rows = pl.ds(pl.multiple_of((far * SPAN + gx) * block + at, size), size)
        remote(own.at[rows], other.at[gx, pl.ds(at, size)], f_send.at[0], f_recv.at[0],
               (s, far * SPAN + gx)).start()

    pass_own(0, block // 2)

    @closing.append
    def _():
        for d in range(SPAN):
            pass_rows(d, 0, block).wait_send()

    diag[...] = jnp.zeros_like(diag)

    def add_diag(j):
        rows = own[pl.ds(pl.multiple_of(j * block, block), block), :]
        diag[...] += dot_t(rows, rows)

    loop(0, n_group, add_diag)
    owner = lax.div(gx, 2)
    slot = lax.rem(gx, 2)

    def diag_copy(d):
        to = lax.rem(k + d, n_k)
        return remote(
            diag.at[pl.ds(pl.multiple_of(to * part, part), part)], diag_in.at[s],
            dr_send.at[d], dr_recv.at[s], (2 * to + owner, g))

    keeps = c == owner
    loop(1, n_k, lambda d: diag_copy(d).start())
    closing.append(lambda: loop(1, n_k, lambda d: diag_copy(d).wait_send()))

    @pl.when(jnp.logical_not(keeps))
    def _():
        diag_copy(0).start()

    mine(0).wait()
    mine(1).wait()
    pass_own(block // 2, block // 2)

    def pass_diag(d):
        return remote(diag_all.at[k, slot], diag_all.at[k, slot], dg_send.at[d], dg_recv.at[slot],
                      x_peer(d))

    @pl.when(keeps)
    def _():
        diag_in[s] = diag[pl.ds(pl.multiple_of(k * part, part), part), :]

        def arrived(d):
            at = lax.rem(s + d, n_space)
            remote(diag.at[pl.ds(0, part)], diag_in.at[at], dr_send.at[0], dr_recv.at[at],
                   (at, g)).wait_recv()

        loop(1, n_space, arrived)
        diag_all[k, slot] = jnp.sum(diag_in[...], axis=0)
        loop(1, SPAN, lambda d: pass_diag(d).start())

    @closing.append
    def _():
        @pl.when(jnp.logical_not(keeps))
        def _():
            diag_copy(0).wait_send()

        @pl.when(keeps)
        def _():
            loop(1, SPAN, lambda d: pass_diag(d).wait_send())

    loop(0, PIECES * SPLIT, send_second)
    loop(0, PIECES - 2, pass_piece)

    def diag_arrived(j):
        @pl.when(2 * c + j != gx)
        def _():
            remote(diag_all.at[k, j], diag_all.at[k, j], dg_send.at[0], dg_recv.at[j],
                   (s, gz * SPAN + 2 * c + j)).wait_recv()

    loop(0, 2, diag_arrived)

    def diag_gather(d):
        return remote(diag_all.at[k], diag_all.at[k], da_send.at[d], da_recv.at[d], core_peer(d))

    loop(1, n_k, lambda d: diag_gather(d).start())
    closing.append(lambda: loop(1, n_k, lambda d: diag_gather(d).wait_send()))
    pass_piece(PIECES - 2)

    class CrossSum:
        def __init__(self, level, cs, cr, cg, ca, all_groups, everyone):
            mid, self.mids, mid_peer = (g, n_group, group_peer) if all_groups else (gx, SPAN, x_peer)
            at, self.peers, peer = (s, n_space, space_peer) if everyone else (k, n_k, core_peer)
            self.cs, self.cr, self.cg, self.ca, self.mid, self.at = cs, cr, cg, ca, mid, at

            def scatter(d):
                to = lax.rem(s + d, n_space)
                return remote(cs.at[to], cr.at[s], r_send.at[level, d], r_recv.at[level, d], (to, g))

            def share(d):
                return remote(cg.at[mid], cg.at[mid], g_send.at[level, d], g_recv.at[level, d], mid_peer(d))

            def gather(d):
                return remote(ca.at[at], ca.at[at], k_send.at[level, d], k_recv.at[level, d], peer(d))

            self.scatter, self.share, self.gather = scatter, share, gather

        def begin(self):
            loop(1, n_space, lambda d: self.scatter(d).start())
            self.cr[s] = self.cs[s]

            @closing.append
            def _():
                loop(1, n_space, lambda d: self.scatter(d).wait_send())
                loop(1, self.mids, lambda d: self.share(d).wait_send())
                loop(1, self.peers, lambda d: self.gather(d).wait_send())

        def to_share(self):
            loop(1, n_space, lambda d: self.scatter(d).wait_recv())
            self.cg[self.mid] = jnp.sum(self.cr[...].astype(F32), axis=0).astype(BF16)
            loop(1, self.mids, lambda d: self.share(d).start())

        def to_gather(self):
            loop(1, self.mids, lambda d: self.share(d).wait_recv())
            self.ca[self.at] = jnp.sum(self.cg[...].astype(F32), axis=0).astype(BF16)
            loop(1, self.peers, lambda d: self.gather(d).start())

        def end(self):
            loop(1, self.peers, lambda d: self.gather(d).wait_recv())

    def mixed(a, b, mix, dst):
        for j in range(block // TILE):
            rows = pl.ds(j * TILE, TILE)
            dst[rows, :] = (dot(a[rows, :], mix[:width, :]) + dot(b[rows, :], mix[width:, :])).astype(BF16)

    def nothing():
        pass

    def filtered(scale, squares, cross, test, midway=nothing):
        start_of_filter(scale, squares, cross, it)

        def step(_):
            filter_step(it, low, square)

        loop(0, 2, step)
        midway()
        loop(2, STEPS - 1, step)
        return mix_of(it[...], test)

    def keep(into, upper, cross, lower):
        into[:width, :width] = upper
        into[width:, width:] = lower
        into[:width, width:] = cross
        into[width:, :width] = cross.T

    for d in (1, 2, 3):
        second(d).wait_recv()
    first_last = PIECES - 1
    for d in (1, 2, 3):
        first(d, first_last).wait_recv()
    sum0 = CrossSum(0, cs0, cr0, cg0, ca0, False, False)
    sum1 = CrossSum(1, cs1, cr1, cg1, ca1, False, False)
    sum2 = CrossSum(2, cs2, cr2, cg2, ca2, True, True)

    def raw_cross(a, b):
        cross = dot_t(panels[0, a], panels[0, b]) + dot_t(panels[1, a], panels[1, b])
        return cross.astype(BF16).reshape(n_k, part, width)

    for i in range(2):
        cross = raw_cross(2 * i, 2 * i + 1)
        for kk in range(n_k):
            cs0[2 * kk + i] = cross[kk]
    sum0.begin()
    for i in range(2):
        for j in range(2):
            cross = raw_cross(i, 2 + j)
            for kk in range(n_k):
                cs1[2 * kk + i, j] = cross[kk]
    sum1.begin()
    sum0.to_share()
    loop(1, n_k, lambda d: diag_gather(d).wait_recv())
    sum0.to_gather()
    for d in (2, 1, 3):
        pass_rows(d, first_last * piece, piece).start()
    sum1.to_share()
    tests.wait()
    upper, lower = (diag_all[:, j].reshape(width, width) for j in range(2))
    scale, squares = diagonal_of_filter(upper, lower, it)
    sum0.end()

    cross = ca0[...].astype(F32).reshape(width, width)
    mix0[0, c] = filtered(scale, squares, cross, sketch[0], sum1.to_gather)
    swap0 = remote(mix0.at[0, c], mix0.at[0, c], c_send.at[0], c_recv.at[0], partner)
    swap0.start()
    mixes = remote(mix0.at[0, c], mix0.at[1, c], z_send.at[0], z_recv.at[0], z_peer(c))
    mixes.start()

    keep(gram, *(diag_all[:, 0].reshape(width, width), ca0[...].astype(F32).reshape(width, width),
                 diag_all[:, 1].reshape(width, width)))
    block1[c] = projected(gram[...], mix0[0, c])
    swap1 = remote(block1.at[c], block1.at[c], c_send.at[1], c_recv.at[1], partner)
    swap1.start()
    mixed(panels.at[gz, 2 * c], panels.at[gz, 2 * c + 1], mix0.at[0, c], pf.at[gz, c])
    swap0.wait_recv()
    mixed(panels.at[gz, 2 - 2 * c], panels.at[gz, 3 - 2 * c], mix0.at[0, 1 - c], pf.at[gz, 1 - c])
    swap1.wait_recv()
    scale, squares = diagonal_of_filter(block1[0], block1[1], it)
    sum1.end()
    raw = ca1[...]
    high, rest = split(
        dot(raw[:, 0].reshape(width, width), mix0[0, 1, :width, :])
        + dot(raw[:, 1].reshape(width, width), mix0[0, 1, width:, :]))
    left = mix0[0, 0, pl.ds(pl.multiple_of(c * width, width), width), :]
    cross1[c] = dot_t(left, high) + dot_t(left, rest)
    swap2 = remote(cross1.at[c], cross1.at[c], c_send.at[2], c_recv.at[2], partner)
    swap2.start()
    swap2.wait_recv()
    mix1[0] = filtered(scale, squares, cross1[0] + cross1[1], sketch[1])
    my_half = pl.ds(pl.multiple_of(c * width, width), width)
    merges = remote(mix1.at[0, my_half], mix1.at[1, my_half], z_send.at[1], z_recv.at[1], z_peer(c))
    merges.start()
    keep(gram1, block1[0], cross1[0] + cross1[1], block1[1])
    block2[gz] = projected(gram1[...], mix1[0])
    strip = pl.ds(pl.multiple_of(c * (width // 2), width // 2), width // 2)
    strips = remote(block2.at[gz, strip], block2.at[gz, strip], e_send.at[0], e_recv.at[0], z_peer(c))
    strips.start()
    mixes.wait_recv()
    swap3 = remote(mix0.at[1, c], mix0.at[1, c], c_send.at[3], c_recv.at[3], partner)
    swap3.start()

    mixed(pf.at[gz, 0], pf.at[gz, 1], mix1.at[0], q.at[gz])
    for d in range(SPAN):
        pass_rows(d, 0, block).wait_recv()
    mixed(other.at[2 * c], other.at[2 * c + 1], mix0.at[1, c], pf.at[far, c])
    swap3.wait_recv()
    mixed(other.at[2 - 2 * c], other.at[3 - 2 * c], mix0.at[1, 1 - c], pf.at[far, 1 - c])
    merges.wait_recv()
    swap4 = remote(mix1.at[1, my_half], mix1.at[1, my_half], c_send.at[4], c_recv.at[4], partner)
    swap4.start()
    swap4.wait_recv()
    mixed(pf.at[far, 0], pf.at[far, 1], mix1.at[1], q.at[far])

    @closing.append
    def _():
        for copy in (swap0, swap1, swap2, swap3, swap4, mixes, merges, strips):
            copy.wait_send()

    cs2[...] = dot_t(q[0], q[1]).astype(BF16).reshape(n_space, part // 2, width)
    sum2.begin()
    remote(block2.at[far, strip], block2.at[far, strip], e_send.at[0], e_recv.at[0], z_peer(c)).wait_recv()
    swap5 = remote(block2.at[far, strip], block2.at[far, strip], e_send.at[1], e_recv.at[1], partner)
    swap5.start()
    closing.append(swap5.wait_send)
    sum2.to_share()
    sum2.to_gather()
    swap5.wait_recv()
    scale, squares = diagonal_of_filter(block2[0], block2[1], it)
    sum2.end()
    last = filtered(scale, squares, ca2[...].astype(F32).reshape(width, width), sketch[2])
    upper, lower = last[:width, :], last[width:, :]
    for j in range(block // TILE):
        rows = pl.ds(j * TILE, TILE)
        out_ref[rows, :] = (dot(q[0, rows, :], upper) + dot(q[1, rows, :], lower)).astype(BF16)
    finish()


def body(n_space, n_group, snapshot_basis, sketch):
    rows, width = snapshot_basis.shape
    block = rows // n_group
    n_k = n_space // 2
    part = width // n_k
    dma = pltpu.SemaphoreType.DMA
    vmem = pltpu.VMEM
    thin = part // 2
    scratch = [
        vmem((2, SPAN, block, width), BF16), vmem((SPAN, block, width), BF16), vmem((rows, width), BF16),
        vmem(sketch.shape, F32),
        vmem((width, width), F32), vmem((n_space, part, width), F32), vmem((n_k, 2, part, width), F32),
        vmem((n_space, part, width), BF16), vmem((n_space, part, width), BF16),
        vmem((SPAN, part, width), BF16), vmem((n_k, part, width), BF16),
        vmem((n_space, 2, part, width), BF16), vmem((n_space, 2, part, width), BF16),
        vmem((SPAN, 2, part, width), BF16), vmem((n_k, 2, part, width), BF16),
        vmem((n_space, thin, width), BF16), vmem((n_space, thin, width), BF16),
        vmem((n_group, thin, width), BF16), vmem((n_space, thin, width), BF16),
        vmem((2 * width, 2 * width), F32), vmem((2 * width, 2 * width), F32), vmem((2 * width, 2 * width), F32),
        vmem((2 * width, 2 * width), BF16), vmem((2 * width, 2 * width), BF16),
        vmem((2, 2, 2 * width, width), BF16), vmem((2, 2 * width, width), BF16),
        vmem((2, 2, block, width), BF16), vmem((2, block, width), BF16),
        vmem((2, width, width), F32), vmem((2, width, width), F32), vmem((2, width, width), F32),
        dma((3, PIECES)), dma((3, PIECES)), dma((3,)), dma((3,)), dma((SPAN,)), dma((SPAN,)), dma((4,)),
        dma((n_k,)), dma((n_space,)), dma((SPAN,)), dma((2,)), dma((n_k,)), dma((n_k,)),
        dma((3, n_space)), dma((3, n_space)), dma((3, n_group)), dma((3, n_group)),
        dma((3, n_space)), dma((3, n_space)), dma((5,)), dma((5,)), dma((2,)), dma((2,)), dma((2,)), dma((2,)),
    ]
    return pl.pallas_call(
        functools.partial(kernel, n_space, n_group),
        out_shape=jax.ShapeDtypeStruct((block, width), BF16),
        in_specs=[pl.BlockSpec(memory_space=pl.ANY)] * 2,
        out_specs=pl.BlockSpec(memory_space=pltpu.VMEM),
        scratch_shapes=scratch,
        compiler_params=pltpu.CompilerParams(
            collective_id=0, has_side_effects=True, vmem_limit_bytes=53 * 1024 * 1024),
        name="merge",
    )(snapshot_basis, sketch)


def solution(mesh):
    in_specs = (P("space", "group"), P())
    out_specs = P(("space", "group"), None)
    step = functools.partial(body, mesh.shape["space"], mesh.shape["group"])
    return jax.shard_map(step, mesh=mesh, in_specs=in_specs, out_specs=out_specs, check_vma=False)
```

```python
import functools

import jax
import jax.numpy as jnp
from jax import lax
from jax.experimental import pallas as pl
from jax.experimental.pallas import tpu as pltpu
from jax.sharding import PartitionSpec as P

STEPS = 5
MESH = pl.DeviceIdType.MESH
F32 = jnp.float32
BF16 = jnp.bfloat16
SPAN = 4
PIECES = 8
SPLIT = 1
TILE = 512


def dot(a, b):
    return jnp.dot(a, b, preferred_element_type=F32)


def dot_t(a, b):
    return lax.dot_general(a, b, (((0,), (0,)), ((), ())), preferred_element_type=F32)


def split(a):
    high = a.astype(BF16)
    return high, (a - high.astype(F32)).astype(BF16)


def loop(low, high, body):
    def step(i, carry):
        body(i)
        return carry

    lax.fori_loop(low, high, step, 0)


def total(a):
    return jnp.sum(a, axis=(0, 1), keepdims=True)


def diagonal_of_filter(upper, lower, into):
    width = upper.shape[0]
    row = lax.broadcasted_iota(jnp.int32, upper.shape, 0)
    col = lax.broadcasted_iota(jnp.int32, upper.shape, 1)
    eye = row == col
    scale = 1.0 / (total(jnp.where(eye, upper + lower, 0.0)) / (2 * width))
    one = jnp.where(eye, 1.0, 0.0)
    upper = upper * scale - one
    lower = lower * scale - one
    into[:width, :width] = upper
    into[width:, width:] = lower
    return scale, total(upper * upper + lower * lower)


def start_of_filter(scale, squares, cross, into):
    width = cross.shape[0]
    cross = cross * scale
    factor = 1.0 / (1.0 + jnp.sqrt(squares + 2.0 * total(cross * cross)))
    cross = cross * factor
    into[:width, width:] = cross
    into[width:, :width] = cross.T
    into[:width, :width] = into[:width, :width] * factor
    into[width:, width:] = into[width:, width:] * factor


def filter_step(iterate, low, square):
    width = iterate.shape[0] // 2
    a, b = pl.ds(0, width), pl.ds(width, width)
    low[...] = iterate[...].astype(BF16)
    square[a, :] = dot(low[a, :], low[...]).astype(BF16)
    square[b, b] = dot(low[b, :], low[:, b]).astype(BF16)
    square[b, a] = square[a, b].T
    top = dot(square[a, :], low[...])
    corner = dot(square[b, :], low[:, b])
    iterate[a, :] = 1.5 * iterate[a, :] - 0.5 * top
    iterate[b, b] = 1.5 * iterate[b, b] - 0.5 * corner
    iterate[b, a] = iterate[a, b].T


def mix_of(iterate, sketch):
    low = iterate.astype(BF16)
    once = dot(low, sketch.astype(BF16))
    twice = dot(low, once.astype(BF16))
    thrice = dot(low, twice.astype(BF16))
    return (0.5 * (sketch + 1.5 * once - 0.5 * thrice)).astype(BF16)


def projected(gram, mix):
    high, low = split(gram)
    half = dot(high, mix) + dot(low, mix)
    high, low = split(half)
    return dot_t(mix, high) + dot_t(mix, low)


def kernel(
    n_space, n_group,
    x_hbm, sk_hbm, out_ref,
    panels, other, own, sketch, diag, diag_in, diag_all,
    cs0, cn0, cb0, cr0, cg0, ca0, cs1, cn1, cb1, cr1, cg1, ca1, cs2, cr2, cg2, ca2,
    gram, gram1, it, low, square, mix0, mix1, pf, q, block1, cross1, block2,
    a_send, a_recv, b_send, b_recv, f_send, f_recv, l_sem,
    dr_send, dr_recv, dg_send, dg_recv, da_send, da_recv,
    r_send, r_recv, g_send, g_recv, k_send, k_recv, c_send, c_recv, z_send, z_recv, e_send, e_recv,
):
    s = lax.axis_index("space")
    g = lax.axis_index("group")
    width = x_hbm.shape[1]
    block = x_hbm.shape[0] // n_group
    n_k = n_space // 2
    k = lax.div(s, 2)
    c = lax.rem(s, 2)
    gx = lax.rem(g, SPAN)
    gz = lax.div(g, SPAN)
    far = 1 - gz
    part = width // n_k
    partner = (2 * k + 1 - c, g)

    def remote(src, dst, send, recv, to):
        return pltpu.make_async_remote_copy(
            src_ref=src, dst_ref=dst, send_sem=send, recv_sem=recv,
            device_id=to, device_id_type=MESH,
        )

    def group_peer(d):
        return s, lax.rem(g + d, n_group)

    def x_peer(d):
        return s, gz * SPAN + lax.rem(gx + d, SPAN)

    def space_peer(d):
        return lax.rem(s + d, n_space), g

    def core_peer(d):
        return 2 * lax.rem(k + d, n_k) + c, g

    def z_peer(core):
        return lax.rem(s - c + n_space // 2, n_space) + core, far * SPAN + gx

    closing = []

    def finish():
        for close in closing:
            close()

    barrier = pltpu.get_barrier_semaphore()

    def greet(to):
        pl.semaphore_signal(barrier, inc=1, device_id=to, device_id_type=MESH)

    loop(1, n_group, lambda d: greet(group_peer(d)))
    loop(1, n_space, lambda d: greet(space_peer(d)))
    loop(0, 2, lambda core: greet(z_peer(core)))

    whole = pltpu.make_async_copy(x_hbm, own, l_sem.at[0])
    whole.start()

    def block_rows(h, x):
        return pl.ds(pl.multiple_of((h * SPAN + x) * block, block), block)

    def mine(h):
        return pltpu.make_async_copy(x_hbm.at[block_rows(h, gx)], panels.at[h, gx], l_sem.at[1 + h])

    mine(0).start()
    mine(1).start()
    tests = pltpu.make_async_copy(sk_hbm, sketch, l_sem.at[3])
    tests.start()
    pl.semaphore_wait(barrier, n_group - 1 + n_space - 1 + 2)

    piece = block // PIECES

    def x_copy(d, h, at, size, send, recv):
        to = lax.rem(gx + d, SPAN)
        return remote(
            own.at[pl.ds(pl.multiple_of((h * SPAN + to) * block + at, size), size)],
            panels.at[h, gx, pl.ds(pl.multiple_of(at, size), size)],
            send, recv, (s, gz * SPAN + to))

    def first(d, p):
        return x_copy(d, far, p * piece, piece, a_send.at[d - 1, p], a_recv.at[d - 1, p])

    def second(d):
        return x_copy(d, gz, 0, block, b_send.at[d - 1], b_recv.at[d - 1])

    def send_first(j):
        p = lax.div(j, SPLIT)
        for d in (2, 1, 3):
            x_copy(d, far, j * (piece // SPLIT), piece // SPLIT,
                   a_send.at[d - 1, p], a_recv.at[d - 1, p]).start()

    def send_second(j):
        for d in (2, 1, 3):
            x_copy(d, gz, j * (piece // SPLIT), piece // SPLIT,
                   b_send.at[d - 1], b_recv.at[d - 1]).start()

    whole.wait()
    loop(0, PIECES * SPLIT, send_first)

    @closing.append
    def _():
        for d in (1, 2, 3):
            loop(0, PIECES, lambda p: first(d, p).wait_send())
            second(d).wait_send()

    def pass_rows(d, at, size):
        x = lax.rem(gx - d + SPAN, SPAN)
        rows = pl.ds(pl.multiple_of(at, size), size)
        return remote(panels.at[far, x, rows], other.at[x, rows], f_send.at[d], f_recv.at[d],
                      (s, far * SPAN + gx))

    def pass_piece(p):
        for d in (2, 1, 3):
            first(d, p).wait_recv()
            pass_rows(d, p * piece, piece).start()

    def pass_own(at, size):
        rows = pl.ds(pl.multiple_of((far * SPAN + gx) * block + at, size), size)
        remote(own.at[rows], other.at[gx, pl.ds(at, size)], f_send.at[0], f_recv.at[0],
               (s, far * SPAN + gx)).start()

    pass_own(0, block // 2)

    @closing.append
    def _():
        for d in range(SPAN):
            pass_rows(d, 0, block).wait_send()

    diag[...] = jnp.zeros_like(diag)

    def add_diag(j):
        rows = own[pl.ds(pl.multiple_of(j * block, block), block), :]
        diag[...] += dot_t(rows, rows)

    loop(0, n_group, add_diag)
    owner = lax.div(gx, 2)
    slot = lax.rem(gx, 2)

    def diag_copy(d):
        to = lax.rem(k + d, n_k)
        return remote(
            diag.at[pl.ds(pl.multiple_of(to * part, part), part)], diag_in.at[s],
            dr_send.at[d], dr_recv.at[s], (2 * to + owner, g))

    keeps = c == owner
    loop(1, n_k, lambda d: diag_copy(d).start())
    closing.append(lambda: loop(1, n_k, lambda d: diag_copy(d).wait_send()))

    @pl.when(jnp.logical_not(keeps))
    def _():
        diag_copy(0).start()

    mine(0).wait()
    mine(1).wait()
    pass_own(block // 2, block // 2)

    def pass_diag(d):
        return remote(diag_all.at[k, slot], diag_all.at[k, slot], dg_send.at[d], dg_recv.at[slot],
                      x_peer(d))

    @pl.when(keeps)
    def _():
        diag_in[s] = diag[pl.ds(pl.multiple_of(k * part, part), part), :]

        def arrived(d):
            at = lax.rem(s + d, n_space)
            remote(diag.at[pl.ds(0, part)], diag_in.at[at], dr_send.at[0], dr_recv.at[at],
                   (at, g)).wait_recv()

        loop(1, n_space, arrived)
        diag_all[k, slot] = jnp.sum(diag_in[...], axis=0)
        loop(1, SPAN, lambda d: pass_diag(d).start())

    @closing.append
    def _():
        @pl.when(jnp.logical_not(keeps))
        def _():
            diag_copy(0).wait_send()

        @pl.when(keeps)
        def _():
            loop(1, SPAN, lambda d: pass_diag(d).wait_send())

    loop(0, PIECES * SPLIT, send_second)
    loop(0, PIECES - 2, pass_piece)

    def diag_arrived(j):
        @pl.when(2 * c + j != gx)
        def _():
            remote(diag_all.at[k, j], diag_all.at[k, j], dg_send.at[0], dg_recv.at[j],
                   (s, gz * SPAN + 2 * c + j)).wait_recv()

    loop(0, 2, diag_arrived)

    def diag_gather(d):
        return remote(diag_all.at[k], diag_all.at[k], da_send.at[d], da_recv.at[d], core_peer(d))

    loop(1, n_k, lambda d: diag_gather(d).start())
    closing.append(lambda: loop(1, n_k, lambda d: diag_gather(d).wait_send()))
    pass_piece(PIECES - 2)

    class CrossSum:
        def __init__(self, level, cs, cr, cg, ca, all_groups, everyone, both_cores=True):
            mid, self.mids, mid_peer = (g, n_group, group_peer) if all_groups else (gx, SPAN, x_peer)
            at, self.peers, peer = (s, n_space, space_peer) if everyone else (k, n_k, core_peer)
            self.cs, self.cr, self.cg, self.ca, self.mid, self.at = cs, cr, cg, ca, mid, at
            self.own, self.senders = (s, n_space) if both_cores else (k, n_k)

            def scatter(d):
                to = lax.rem(self.own + d, self.senders)
                return remote(cs.at[to], cr.at[self.own], r_send.at[level, d], r_recv.at[level, d],
                              space_peer(d) if both_cores else core_peer(d))

            def share(d):
                return remote(cg.at[mid], cg.at[mid], g_send.at[level, d], g_recv.at[level, d], mid_peer(d))

            def gather(d):
                return remote(ca.at[at], ca.at[at], k_send.at[level, d], k_recv.at[level, d], peer(d))

            self.scatter, self.share, self.gather = scatter, share, gather

        def begin(self):
            loop(1, self.senders, lambda d: self.scatter(d).start())
            self.cr[self.own] = self.cs[self.own]

            @closing.append
            def _():
                loop(1, self.senders, lambda d: self.scatter(d).wait_send())
                loop(1, self.mids, lambda d: self.share(d).wait_send())
                loop(1, self.peers, lambda d: self.gather(d).wait_send())

        def to_share(self):
            loop(1, self.senders, lambda d: self.scatter(d).wait_recv())
            self.cg[self.mid] = jnp.sum(self.cr[...].astype(F32), axis=0).astype(BF16)
            loop(1, self.mids, lambda d: self.share(d).start())

        def to_gather(self):
            loop(1, self.mids, lambda d: self.share(d).wait_recv())
            self.ca[self.at] = jnp.sum(self.cg[...].astype(F32), axis=0).astype(BF16)
            loop(1, self.peers, lambda d: self.gather(d).start())

        def end(self):
            loop(1, self.peers, lambda d: self.gather(d).wait_recv())

    def mixed(a, b, mix, dst):
        for j in range(block // TILE):
            rows = pl.ds(j * TILE, TILE)
            dst[rows, :] = (dot(a[rows, :], mix[:width, :]) + dot(b[rows, :], mix[width:, :])).astype(BF16)

    def nothing():
        pass

    def filtered(scale, squares, cross, test, midway=nothing):
        start_of_filter(scale, squares, cross, it)

        def step(_):
            filter_step(it, low, square)

        loop(0, 2, step)
        midway()
        loop(2, STEPS - 1, step)
        return mix_of(it[...], test)

    def keep(into, upper, cross, lower):
        into[:width, :width] = upper
        into[width:, width:] = lower
        into[:width, width:] = cross
        into[width:, :width] = cross.T

    for d in (1, 2, 3):
        second(d).wait_recv()
    first_last = PIECES - 1
    for d in (1, 2, 3):
        first(d, first_last).wait_recv()
    sum0 = CrossSum(0, cb0, cr0, cg0, ca0, False, False, both_cores=False)
    sum1 = CrossSum(1, cb1, cr1, cg1, ca1, False, False, both_cores=False)
    sum2 = CrossSum(2, cs2, cr2, cg2, ca2, True, True)

    def core_sum(n, both, arriving, kept):
        swap = remote(both.at[1 - c], arriving, c_send.at[n], c_recv.at[n], partner)
        swap.start()
        closing.append(swap.wait_send)
        swap.wait_recv()
        kept[...] = (both[c].astype(F32) + arriving[...].astype(F32)).astype(BF16)

    def raw_cross(a, b):
        cross = dot_t(panels[0, a], panels[0, b]) + dot_t(panels[1, a], panels[1, b])
        return cross.astype(BF16).reshape(n_k, part, width)

    for i in range(2):
        cs0[i] = raw_cross(2 * i, 2 * i + 1)
    core_sum(6, cs0, cn0, cb0)
    sum0.begin()
    for i in range(2):
        for j in range(2):
            cs1[i, :, j] = raw_cross(i, 2 + j)
    core_sum(5, cs1, cn1, cb1)
    sum1.begin()
    sum0.to_share()
    loop(1, n_k, lambda d: diag_gather(d).wait_recv())
    sum0.to_gather()
    for d in (2, 1, 3):
        pass_rows(d, first_last * piece, piece).start()
    sum1.to_share()
    tests.wait()
    upper, lower = (diag_all[:, j].reshape(width, width) for j in range(2))
    scale, squares = diagonal_of_filter(upper, lower, it)
    sum0.end()

    cross = ca0[...].astype(F32).reshape(width, width)
    mix0[0, c] = filtered(scale, squares, cross, sketch[0], sum1.to_gather)
    swap0 = remote(mix0.at[0, c], mix0.at[0, c], c_send.at[0], c_recv.at[0], partner)
    swap0.start()
    mixes = remote(mix0.at[0, c], mix0.at[1, c], z_send.at[0], z_recv.at[0], z_peer(c))
    mixes.start()

    keep(gram, *(diag_all[:, 0].reshape(width, width), ca0[...].astype(F32).reshape(width, width),
                 diag_all[:, 1].reshape(width, width)))
    block1[c] = projected(gram[...], mix0[0, c])
    swap1 = remote(block1.at[c], block1.at[c], c_send.at[1], c_recv.at[1], partner)
    swap1.start()
    mixed(panels.at[gz, 2 * c], panels.at[gz, 2 * c + 1], mix0.at[0, c], pf.at[gz, c])
    swap0.wait_recv()
    mixed(panels.at[gz, 2 - 2 * c], panels.at[gz, 3 - 2 * c], mix0.at[0, 1 - c], pf.at[gz, 1 - c])
    swap1.wait_recv()
    scale, squares = diagonal_of_filter(block1[0], block1[1], it)
    sum1.end()
    raw = ca1[...]
    high, rest = split(
        dot(raw[:, 0].reshape(width, width), mix0[0, 1, :width, :])
        + dot(raw[:, 1].reshape(width, width), mix0[0, 1, width:, :]))
    left = mix0[0, 0, pl.ds(pl.multiple_of(c * width, width), width), :]
    cross1[c] = dot_t(left, high) + dot_t(left, rest)
    swap2 = remote(cross1.at[c], cross1.at[c], c_send.at[2], c_recv.at[2], partner)
    swap2.start()
    swap2.wait_recv()
    mix1[0] = filtered(scale, squares, cross1[0] + cross1[1], sketch[1])
    my_half = pl.ds(pl.multiple_of(c * width, width), width)
    merges = remote(mix1.at[0, my_half], mix1.at[1, my_half], z_send.at[1], z_recv.at[1], z_peer(c))
    merges.start()
    keep(gram1, block1[0], cross1[0] + cross1[1], block1[1])
    block2[gz] = projected(gram1[...], mix1[0])
    strip = pl.ds(pl.multiple_of(c * (width // 2), width // 2), width // 2)
    strips = remote(block2.at[gz, strip], block2.at[gz, strip], e_send.at[0], e_recv.at[0], z_peer(c))
    strips.start()
    mixes.wait_recv()
    swap3 = remote(mix0.at[1, c], mix0.at[1, c], c_send.at[3], c_recv.at[3], partner)
    swap3.start()

    mixed(pf.at[gz, 0], pf.at[gz, 1], mix1.at[0], q.at[gz])
    for d in range(SPAN):
        pass_rows(d, 0, block).wait_recv()
    mixed(other.at[2 * c], other.at[2 * c + 1], mix0.at[1, c], pf.at[far, c])
    swap3.wait_recv()
    mixed(other.at[2 - 2 * c], other.at[3 - 2 * c], mix0.at[1, 1 - c], pf.at[far, 1 - c])
    merges.wait_recv()
    swap4 = remote(mix1.at[1, my_half], mix1.at[1, my_half], c_send.at[4], c_recv.at[4], partner)
    swap4.start()
    swap4.wait_recv()
    mixed(pf.at[far, 0], pf.at[far, 1], mix1.at[1], q.at[far])

    @closing.append
    def _():
        for copy in (swap0, swap1, swap2, swap3, swap4, mixes, merges, strips):
            copy.wait_send()

    cs2[...] = dot_t(q[0], q[1]).astype(BF16).reshape(n_space, part // 2, width)
    sum2.begin()
    remote(block2.at[far, strip], block2.at[far, strip], e_send.at[0], e_recv.at[0], z_peer(c)).wait_recv()
    swap5 = remote(block2.at[far, strip], block2.at[far, strip], e_send.at[1], e_recv.at[1], partner)
    swap5.start()
    closing.append(swap5.wait_send)
    sum2.to_share()
    sum2.to_gather()
    swap5.wait_recv()
    scale, squares = diagonal_of_filter(block2[0], block2[1], it)
    sum2.end()
    last = filtered(scale, squares, ca2[...].astype(F32).reshape(width, width), sketch[2])
    upper, lower = last[:width, :], last[width:, :]
    for j in range(block // TILE):
        rows = pl.ds(j * TILE, TILE)
        out_ref[rows, :] = (dot(q[0, rows, :], upper) + dot(q[1, rows, :], lower)).astype(BF16)
    finish()


def body(n_space, n_group, snapshot_basis, sketch):
    rows, width = snapshot_basis.shape
    block = rows // n_group
    n_k = n_space // 2
    part = width // n_k
    dma = pltpu.SemaphoreType.DMA
    vmem = pltpu.VMEM
    thin = part // 2
    scratch = [
        vmem((2, SPAN, block, width), BF16), vmem((SPAN, block, width), BF16), vmem((rows, width), BF16),
        vmem(sketch.shape, F32),
        vmem((width, width), F32), vmem((n_space, part, width), F32), vmem((n_k, 2, part, width), F32),
        vmem((2, n_k, part, width), BF16), vmem((n_k, part, width), BF16),
        vmem((n_k, part, width), BF16), vmem((n_k, part, width), BF16),
        vmem((SPAN, part, width), BF16), vmem((n_k, part, width), BF16),
        vmem((2, n_k, 2, part, width), BF16), vmem((n_k, 2, part, width), BF16),
        vmem((n_k, 2, part, width), BF16), vmem((n_k, 2, part, width), BF16),
        vmem((SPAN, 2, part, width), BF16), vmem((n_k, 2, part, width), BF16),
        vmem((n_space, thin, width), BF16), vmem((n_space, thin, width), BF16),
        vmem((n_group, thin, width), BF16), vmem((n_space, thin, width), BF16),
        vmem((2 * width, 2 * width), F32), vmem((2 * width, 2 * width), F32), vmem((2 * width, 2 * width), F32),
        vmem((2 * width, 2 * width), BF16), vmem((2 * width, 2 * width), BF16),
        vmem((2, 2, 2 * width, width), BF16), vmem((2, 2 * width, width), BF16),
        vmem((2, 2, block, width), BF16), vmem((2, block, width), BF16),
        vmem((2, width, width), F32), vmem((2, width, width), F32), vmem((2, width, width), F32),
        dma((3, PIECES)), dma((3, PIECES)), dma((3,)), dma((3,)), dma((SPAN,)), dma((SPAN,)), dma((4,)),
        dma((n_k,)), dma((n_space,)), dma((SPAN,)), dma((2,)), dma((n_k,)), dma((n_k,)),
        dma((3, n_space)), dma((3, n_space)), dma((3, n_group)), dma((3, n_group)),
        dma((3, n_space)), dma((3, n_space)), dma((8,)), dma((8,)), dma((2,)), dma((2,)), dma((2,)), dma((2,)),
    ]
    return pl.pallas_call(
        functools.partial(kernel, n_space, n_group),
        out_shape=jax.ShapeDtypeStruct((block, width), BF16),
        in_specs=[pl.BlockSpec(memory_space=pl.ANY)] * 2,
        out_specs=pl.BlockSpec(memory_space=pltpu.VMEM),
        scratch_shapes=scratch,
        compiler_params=pltpu.CompilerParams(
            collective_id=0, has_side_effects=True, vmem_limit_bytes=53 * 1024 * 1024),
        name="merge",
    )(snapshot_basis, sketch)


def solution(mesh):
    in_specs = (P("space", "group"), P())
    out_specs = P(("space", "group"), None)
    step = functools.partial(body, mesh.shape["space"], mesh.shape["group"])
    return jax.shard_map(step, mesh=mesh, in_specs=in_specs, out_specs=out_specs, check_vma=False)
```
